32 devices in a mesh: row: 2 (over y), col: 16 (over z, x, core).
Axes of the slice: x: 2, y: 2, z: 4, core: 2. Of those that a mesh axis runs over, the one named last changes fastest.
Arguments:
- image_student: bfloat16 [2048, 1024], P(('row', 'col')), may hold values from -2.5 to 2.5
- text_student: bfloat16 [2048, 1024], P(('col', 'row')), may hold values from -2.5 to 2.5
- image_teacher: bfloat16 [2048, 1024], P(('row', 'col')), may hold values from -2.5 to 2.5
- text_teacher: bfloat16 [2048, 1024], P(('col', 'row')), may hold values from -2.5 to 2.5
Outputs:
- loss: float32 [], replicated
- image_grad: float32 [2048, 1024], P(('row', 'col'))
- text_grad: float32 [2048, 1024], P(('col', 'row'))
The draws below stay inside these ranges and needn't reach their ends.
All inputs are finite; a program needn't handle non-finite values.
Results may differ from the reference program's by a relative error of at most 0.002.
Values may be sent and summed in bfloat16 or wider, within the bound.
A program may use at most 128 MiB of HBM per device.

```python
import math
import jax
import jax.numpy as jnp
from jax import lax

D = 1024
B = 2048


def embedding(key, which):
    base = jnp.clip(jax.random.normal(jax.random.fold_in(key, which), (B, D), jnp.float32), -5.0, 5.0) / math.sqrt(D)
    return base


def draw_image_student(key, part):
    return embedding(key, 11).astype(jnp.bfloat16)


def draw_text_student(key, part):
    return embedding(key, 12).astype(jnp.bfloat16)


def draw_image_teacher(key, part):
    return embedding(key, 13).astype(jnp.bfloat16)


def draw_text_teacher(key, part):
    return embedding(key, 14).astype(jnp.bfloat16)


def setup_inputs(seed: int = 0) -> dict:
    key_of = jax.random.split(jax.random.key(seed), 5)
    image_student = draw_image_student(jax.random.fold_in(key_of[4], 71), 0)
    text_student = draw_text_student(jax.random.fold_in(key_of[4], 71), 0)
    image_teacher = draw_image_teacher(jax.random.fold_in(key_of[4], 71), 0)
    text_teacher = draw_text_teacher(jax.random.fold_in(key_of[4], 71), 0)
    return dict(image_student=image_student, text_student=text_student, image_teacher=image_teacher, text_teacher=text_teacher)


logit_scale = 100.0

def tile_logits(left, right):
    return logit_scale * lax.dot_general(left.astype(jnp.float32), right.astype(jnp.float32), (((1,), (1,)), ((), ())), preferred_element_type=jnp.float32)

def partial_stats(student, teacher, along):
    student_high = jnp.max(student, along, keepdims=True)
    student_total = jnp.sum(jnp.exp(student - student_high), along)
    teacher_high = jnp.max(teacher, along, keepdims=True)
    weights = jnp.exp(teacher - teacher_high)
    teacher_total = jnp.sum(weights, along)
    divergence = jnp.sum(weights * (teacher - student), along)
    return (jnp.squeeze(student_high, along), student_total, jnp.squeeze(teacher_high, along), teacher_total, divergence)

def merge_stats(first, second):
    student_high = jnp.maximum(first[0], second[0])
    teacher_high = jnp.maximum(first[2], second[2])
    early = jnp.exp(first[2] - teacher_high)
    later = jnp.exp(second[2] - teacher_high)
    student_total = first[1] * jnp.exp(first[0] - student_high) + second[1] * jnp.exp(second[0] - student_high)
    return (student_high, student_total, teacher_high, first[3] * early + second[3] * later, first[4] * early + second[4] * later)

def finish(stats):
    student_lse = stats[0] + jnp.log(stats[1])
    teacher_lse = stats[2] + jnp.log(stats[3])
    divergence = stats[4] / stats[3] - teacher_lse + student_lse
    return (student_lse, teacher_lse, 0.5 * (student_lse + divergence))

def reference(image_student, text_student, image_teacher, text_teacher):
    total = image_student.shape[0]
    width = image_student.shape[1]
    block = math.gcd(total, 512)
    count = total // block
    columns = jnp.arange(total, dtype=jnp.int32)
    starts = jnp.arange(count, dtype=jnp.int32) * block
    image_blocks = image_student.reshape(count, block, width)
    frozen_blocks = image_teacher.reshape(count, block, width)

    def first_pass(carry, inputs):
        image_rows, frozen_rows, start = inputs
        student = tile_logits(image_rows, text_student)
        teacher = tile_logits(frozen_rows, text_teacher)
        row_part = partial_stats(student, teacher, 1)
        merged = merge_stats(carry, partial_stats(student, teacher, 0))
        row_index = start + jnp.arange(block, dtype=jnp.int32)
        identity = (row_index[:, None] == columns[None, :]).astype(jnp.float32)
        return (merged, (row_part, jnp.sum(student * identity)))
    lowest = jnp.full((total,), -1e+30, jnp.float32)
    nothing = jnp.zeros((total,), jnp.float32)
    column_stats, (row_blocks, diagonals) = lax.scan(first_pass, (lowest, nothing, lowest, nothing, nothing), (image_blocks, frozen_blocks, starts))
    row_stats = tuple((member.reshape(total) for member in row_blocks))
    student_rows, teacher_rows, row_terms = finish(row_stats)
    student_columns, teacher_columns, column_terms = finish(column_stats)
    loss = (jnp.sum(row_terms) + jnp.sum(column_terms) - jnp.sum(diagonals)) / total

    def second_pass(text_grad, inputs):
        image_rows, frozen_rows, start, student_lse, teacher_lse = inputs
        student = tile_logits(image_rows, text_student)
        teacher = tile_logits(frozen_rows, text_teacher)
        row_index = start + jnp.arange(block, dtype=jnp.int32)
        identity = (row_index[:, None] == columns[None, :]).astype(jnp.float32)
        gradient = (jnp.exp(student - student_lse[:, None]) + jnp.exp(student - student_columns[None, :]) - 0.5 * (jnp.exp(teacher - teacher_lse[:, None]) + jnp.exp(teacher - teacher_columns[None, :])) - identity).astype(jnp.bfloat16)
        image_part = logit_scale * jnp.dot(gradient.astype(jnp.float32), text_student.astype(jnp.float32), preferred_element_type=jnp.float32)
        text_grad = text_grad + logit_scale * lax.dot_general(gradient.astype(jnp.float32), image_rows.astype(jnp.float32), (((0,), (0,)), ((), ())), preferred_element_type=jnp.float32)
        return (text_grad, image_part)
    text_grad, image_parts = lax.scan(second_pass, jnp.zeros((total, width), jnp.float32), (image_blocks, frozen_blocks, starts, student_rows.reshape(count, block), teacher_rows.reshape(count, block)))
    return (loss, image_parts.reshape(total, width), text_grad)
```

```python
import functools

import jax
import jax.numpy as jnp
from jax import lax
from jax.experimental import pallas as pl
from jax.experimental.pallas import tpu as pltpu
from jax.sharding import PartitionSpec as P

logit_scale = 100.0
MESH = pl.DeviceIdType.MESH
f32, bf16 = jnp.float32, jnp.bfloat16


def layout(mesh_shape):
    rows, cols = mesh_shape["row"], mesh_shape["col"]
    cores = 2 if cols % 2 == 0 else 1
    chips = cols // cores
    divisors = [d for d in range(1, chips + 1) if chips % d == 0]
    a = min(divisors, key=lambda d: d + rows * chips // d)
    q = max(d for d in range(1, a + 1) if a % d == 0 and d * d <= a)
    return dict(R=rows, C=cols, K=cores, A=a, H=chips // a, Q=q, P=a // q)


def contract_last(left, right):
    return lax.dot_general(left, right, (((1,), (1,)), ((), ())), preferred_element_type=f32)


def contract_first(left, right):
    return lax.dot_general(left, right, (((0,), (0,)), ((), ())), preferred_element_type=f32)


def merged(slots, count):
    def line(index, which):
        return slots[index, which : which + 1, :]

    student_high = functools.reduce(jnp.maximum, [line(i, 0) for i in range(count)])
    teacher_high = functools.reduce(jnp.maximum, [line(i, 2) for i in range(count)])
    student_total = teacher_total = divergence = 0.0
    for i in range(count):
        student_total += line(i, 1) * jnp.exp(line(i, 0) - student_high)
        factor = jnp.exp(line(i, 2) - teacher_high)
        teacher_total += line(i, 3) * factor
        divergence += line(i, 4) * factor
    student_lse = student_high + jnp.log(student_total)
    teacher_lse = teacher_high + jnp.log(teacher_total)
    kl = divergence / teacher_total - teacher_lse + student_lse
    return student_lse, teacher_lse, 0.5 * (student_lse + kl)


def position(index, step, count):
    total = jnp.zeros_like(index)
    for t in range(1, count):
        total += (index >= t * step).astype(jnp.int32)
    return total


def kernel(
    g, n_send, total,
    is_hbm, ts_hbm, it_hbm, tt_hbm,
    loss_ref, ig_ref, tg_ref,
    imgs, imgo, imgt, txts, txtt,
    s_ref, t_ref, rowtmp, rstat, cstat, la, lb, gbuf, grecv,
    pi, pib, pt, ptb, ri, rt,
    local_sem, send_sem, rimgs, rimgo, rimgt, rtxts, rtxtt, rrow, rcol, rla, rlb, rg, rri, rrt,
):
    R, K, A, H, Q, PP = g["R"], g["K"], g["A"], g["H"], g["Q"], g["P"]
    n = is_hbm.shape[0]
    r = lax.axis_index("row")
    c = lax.axis_index("col")
    k, chip = lax.rem(c, K), lax.div(c, K)
    lo, hi = lax.rem(chip, A), lax.div(chip, A)
    q, p = lax.rem(lo, Q), lax.div(lo, Q)
    HR, T = H * R, K * H * R

    def dev(r_, hi_, lo_, k_):
        return (r_, (hi_ * A + lo_) * K + k_)

    def up(value, step, count):
        return lax.rem(value + step, count)

    def down(value, step, count):
        return lax.rem(value + count - step, count)

    def block(ref, index):
        return ref.at[pl.ds(pl.multiple_of(index * n, n), n), :]

    a_peers = [dev(r, hi, up(lo, d, A), k) for d in range(1, A)]
    b_steps = [(dk, dh, dr) for dk in range(K) for dh in range(H) for dr in range(R)]
    b_peers = [dev(up(r, dr, R), up(hi, dh, H), lo, up(k, dk, K)) for dk, dh, dr in b_steps[1:]]
    partner = dev(r, hi, lo, up(k, 1, K))

    pending = []

    def send(src, dst, recv, target):
        copy = pltpu.make_async_remote_copy(
            src_ref=src, dst_ref=dst, send_sem=send_sem.at[len(pending)], recv_sem=recv,
            device_id=target, device_id_type=MESH,
        )
        copy.start()
        pending.append(copy)

    def arrived(ref, recv):
        pltpu.make_async_remote_copy(
            src_ref=ref, dst_ref=ref, send_sem=send_sem.at[0], recv_sem=recv,
            device_id=partner, device_id_type=MESH,
        ).wait_recv()

    own_text = (k * H + hi) * R + r
    loads = []
    for i, (src, dst) in enumerate((
        (is_hbm, block(imgs, lo)), (ts_hbm, block(txts, own_text)),
        (it_hbm, block(imgt, lo)), (tt_hbm, block(txtt, own_text)),
    )):
        copy = pltpu.make_async_copy(src, dst, local_sem.at[i])
        copy.start()
        loads.append(copy)
    barrier = pltpu.get_barrier_semaphore()
    for target in a_peers + b_peers:
        pl.semaphore_signal(barrier, inc=1, device_id=target, device_id_type=MESH)
    pl.semaphore_wait(barrier, len(a_peers) + len(b_peers))

    def image_slot(dp, dq):
        return down(p, dp, PP) * Q + down(q, dq, Q)

    def text_slot(dk, dh, dr):
        return (down(k, dk, K) * H + down(hi, dh, H)) * R + down(r, dr, R)

    def image_own(ref, sems):
        for dp in range(1, PP):
            send(block(ref, lo), block(ref, lo), sems.at[dp * Q], dev(r, hi, up(p, dp, PP) * Q + q, k))

    def image_spread(ref, sems, dp):
        slot = image_slot(dp, 0)
        for dq in range(1, Q):
            send(block(ref, slot), block(ref, slot), sems.at[dp * Q + dq],
                 dev(r, hi, p * Q + up(q, dq, Q), k))

    def text_own(ref, sems):
        for dh in range(1, H):
            send(block(ref, own_text), block(ref, own_text), sems.at[dh * R],
                 dev(r, up(hi, dh, H), lo, k))

    def text_spread(ref, sems, dh):
        slot = text_slot(0, dh, 0)
        for dr in range(1, R):
            send(block(ref, slot), block(ref, slot), sems.at[dh * R + dr],
                 dev(up(r, dr, R), hi, lo, k))

    def text_across(ref, sems, dh, dr):
        slot = text_slot(0, dh, dr)
        for dk in range(1, K):
            send(block(ref, slot), block(ref, slot), sems.at[(dk * H + dh) * R + dr],
                 dev(r, hi, lo, up(k, dk, K)))

    pairs = ((imgs, rimgs, txts, rtxts), (imgt, rimgt, txtt, rtxtt))
    for i, (img, rimg, txt, rtxt) in enumerate(pairs):
        loads[2 * i].wait()
        image_own(img, rimg)
        loads[2 * i + 1].wait()
        text_own(txt, rtxt)
        image_spread(img, rimg, 0)
        text_spread(txt, rtxt, 0)
        text_across(txt, rtxt, 0, 0)

    def forward(img, rimg, txt, rtxt):
        for dp in range(1, PP):
            arrived(block(img, image_slot(dp, 0)), rimg.at[dp * Q])
            image_spread(img, rimg, dp)
        for dh in range(1, H):
            arrived(block(txt, text_slot(0, dh, 0)), rtxt.at[dh * R])
            text_spread(txt, rtxt, dh)
            text_across(txt, rtxt, dh, 0)

    def collect(img, rimg, txt, rtxt):
        for dh in range(H):
            for dr in range(1, R):
                arrived(block(txt, text_slot(0, dh, dr)), rtxt.at[dh * R + dr])
                text_across(txt, rtxt, dh, dr)
        for dp in range(PP):
            for dq in range(1, Q):
                arrived(block(img, image_slot(dp, dq)), rimg.at[dp * Q + dq])
        for dk, dh, dr in b_steps:
            if dk:
                arrived(block(txt, text_slot(dk, dh, dr)), rtxt.at[(dk * H + dh) * R + dr])

    for pair in pairs:
        forward(*pair)
    collect(*pairs[0])
    s_ref[...] = logit_scale * contract_last(imgs[...], txts[...])
    collect(*pairs[1])
    if K > 1:
        send(imgs, imgo, rimgo, partner)
    t_ref[...] = logit_scale * contract_last(imgt[...], txtt[...])

    rows, width = s_ref.shape
    col_s = jnp.max(s_ref[...], axis=0, keepdims=True)
    col_t = jnp.max(t_ref[...], axis=0, keepdims=True)
    lane = lax.broadcasted_iota(jnp.int32, (n, 128), 1)
    col_id = lax.broadcasted_iota(jnp.int32, (1, width), 1)
    col_slot = position(col_id, n, T)
    slot_k, slot_h = position(col_slot, HR, K), position(col_slot, R, K * H)
    slot_r = col_slot - slot_h * R
    slot_h = slot_h - slot_k * H
    col_id = (((slot_h * A + lo) * K + slot_k) * R + slot_r) * n + col_id - col_slot * n
    row_id = lax.broadcasted_iota(jnp.int32, (n, 1), 0)
    sums = [0.0] * 3
    diagonal = 0.0

    def eye(b):
        base = (r * g["C"] + (hi * A + b) * K + k) * n
        return row_id + base == col_id

    for b in range(A):
        at = slice(b * n, (b + 1) * n)
        s, t = s_ref[at, :], t_ref[at, :]
        gap = t - s
        row_s = jnp.max(s, axis=1, keepdims=True)
        row_t = jnp.max(t, axis=1, keepdims=True)
        row_weight = jnp.exp(t - row_t)
        stats = (
            row_s,
            jnp.sum(jnp.exp(s - row_s), axis=1, keepdims=True),
            row_t,
            jnp.sum(row_weight, axis=1, keepdims=True),
            jnp.sum(row_weight * gap, axis=1, keepdims=True),
        )
        packed = jnp.zeros((n, 128), f32)
        for i, value in enumerate(stats):
            packed = jnp.where(lane == i, value, packed)
        rowtmp[at, :] = packed
        col_weight = jnp.exp(t - col_t)
        parts = (jnp.exp(s - col_s), col_weight, col_weight * gap)
        sums = [old + jnp.sum(new, axis=0, keepdims=True) for old, new in zip(sums, parts)]
        diagonal += jnp.sum(jnp.where(eye(b), s, 0.0), axis=0, keepdims=True)
    line = lax.broadcasted_iota(jnp.int32, (8, width), 0)
    packed = jnp.zeros((8, width), f32)
    for i, value in enumerate((col_s, sums[0], col_t, sums[1], sums[2])):
        packed = jnp.where(line == i, value, packed)
    cstat[0] = packed
    for e, target in enumerate(b_peers, 1):
        send(cstat.at[0], cstat.at[e], rcol.at[e], target)
    rstat[0] = jnp.transpose(rowtmp[...])[:8, :]
    for d, target in enumerate(a_peers, 1):
        send(rstat.at[0], rstat.at[d], rrow.at[d], target)
    for d in range(1, A):
        arrived(rstat.at[d], rrow.at[d])
    row_student, row_teacher, row_terms = merged(rstat, A)
    line = lax.broadcasted_iota(jnp.int32, (128, rows), 0)
    rowtmp[...] = jnp.transpose(jnp.where(line == 0, row_student, row_teacher))
    for e in range(1, T):
        arrived(cstat.at[e], rcol.at[e])
    col_student, col_teacher, col_terms = merged(cstat, T)

    at_row = lax.broadcasted_iota(jnp.int32, (1, rows), 1) - lo * n
    at_col = lax.broadcasted_iota(jnp.int32, (1, width), 1) - own_text * n
    share = (
        jnp.sum(jnp.where((at_row >= 0) & (at_row < n), row_terms, 0.0), axis=1, keepdims=True)
        + jnp.sum(
            jnp.where((at_col >= 0) & (at_col < n), col_terms, 0.0) - diagonal,
            axis=1, keepdims=True,
        )
    )
    la[0] = jnp.broadcast_to(share, (8, 128))
    for d, target in enumerate(a_peers, 1):
        send(la.at[0], la.at[d], rla.at[d], target)

    half = width // K
    for b in range(A):
        at = slice(b * n, (b + 1) * n)
        s, t = s_ref[at, :], t_ref[at, :]
        row_s, row_t = rowtmp[at, 0:1], rowtmp[at, 1:2]
        grad = (
            jnp.exp(s - row_s) + jnp.exp(s - col_student)
            - 0.5 * (jnp.exp(t - row_t) + jnp.exp(t - col_teacher))
            - jnp.where(eye(b), 1.0, 0.0)
        ).astype(bf16)
        for j in range(K):
            gbuf[j, at, :] = grad[:, j * half : (j + 1) * half]
    if K > 1:
        send(gbuf.at[up(k, 1, K)], grecv, rg, partner)

    partial = 0.0
    for j in range(K):
        partial += jnp.dot(gbuf[j], txts[j * half : (j + 1) * half, :], preferred_element_type=f32)
    pi[...] = partial
    pib[...] = partial.astype(bf16)
    for d, target in enumerate(a_peers, 1):
        send(block(pib, up(lo, d, A)), ri.at[d - 1], rri.at[d], target)

    for d in range(1, A):
        arrived(la.at[d], rla.at[d])
    lb[0] = functools.reduce(jnp.add, [la[d] for d in range(A)])
    for e, target in enumerate(b_peers, 1):
        send(lb.at[0], lb.at[e], rlb.at[e], target)

    if K > 1:
        arrived(imgo, rimgo)
        arrived(grecv, rg)
    partial = contract_first(gbuf[k], imgs[...])
    if K > 1:
        partial += contract_first(grecv[...], imgo[...])
    pt[...] = partial
    ptb[...] = partial.astype(bf16)
    for dh in range(H):
        for dr in range(R):
            if dh or dr:
                send(block(ptb, up(hi, dh, H) * R + up(r, dr, R)), rt.at[dh * R + dr - 1],
                     rrt.at[dh * R + dr], dev(up(r, dr, R), up(hi, dh, H), lo, k))

    for e in range(1, T):
        arrived(lb.at[e], rlb.at[e])
    loss_ref[...] = functools.reduce(jnp.add, [lb[e] for e in range(T)]) / total
    for d in range(1, A):
        arrived(ri.at[d - 1], rri.at[d])
    value = block(pi, lo)[...]
    for d in range(1, A):
        value += ri[d - 1].astype(f32)
    ig_ref[...] = logit_scale * value
    for e in range(1, HR):
        arrived(rt.at[e - 1], rrt.at[e])
    value = block(pt, hi * R + r)[...]
    for e in range(1, HR):
        value += rt[e - 1].astype(f32)
    tg_ref[...] = logit_scale * value
    for copy in pending:
        copy.wait_send()
    assert len(pending) == n_send, len(pending)


def solution(mesh):
    g = layout(mesh.shape)
    R, K, A, H, Q, PP = g["R"], g["K"], g["A"], g["H"], g["Q"], g["P"]
    HR, T = H * R, K * H * R
    gather = 2 * (A - 1) + 2 * (HR - 1) + 2 * HR * (K - 1) + (K - 1)
    n_send = gather + 2 * (A - 1) + 2 * (T - 1) + (K - 1) + (A - 1) + (HR - 1)

    def body(image_student, text_student, image_teacher, text_teacher):
        n, width = image_student.shape
        rows, cols = A * n, T * n
        total = n * R * g["C"]
        vmem, dma = pltpu.VMEM, pltpu.SemaphoreType.DMA
        block_out = jax.ShapeDtypeStruct((n, width), f32)
        loss, image_grad, text_grad = pl.pallas_call(
            functools.partial(kernel, g, n_send, total),
            out_shape=(jax.ShapeDtypeStruct((8, 128), f32), block_out, block_out),
            in_specs=[pl.BlockSpec(memory_space=pl.ANY)] * 4,
            out_specs=[pl.BlockSpec(memory_space=pltpu.VMEM)] * 3,
            scratch_shapes=[
                vmem((rows, width), bf16), vmem((rows, width), bf16), vmem((rows, width), bf16),
                vmem((cols, width), bf16), vmem((cols, width), bf16),
                vmem((rows, cols), f32), vmem((rows, cols), f32),
                vmem((rows, 128), f32), vmem((A, 8, rows), f32), vmem((T, 8, cols), f32),
                vmem((A, 8, 128), f32), vmem((T, 8, 128), f32),
                vmem((K, rows, cols // K), bf16), vmem((rows, cols // K), bf16),
                vmem((rows, width), f32), vmem((rows, width), bf16),
                vmem((cols // K, width), f32), vmem((cols // K, width), bf16),
                vmem((max(A - 1, 1), n, width), bf16), vmem((max(HR - 1, 1), n, width), bf16),
                dma((4,)), dma((n_send,)),
                dma((A,)), dma(()), dma((A,)), dma((T,)), dma((T,)),
                dma((A,)), dma((T,)), dma((A,)), dma((T,)), dma(()), dma((A,)), dma((HR,)),
            ],
            compiler_params=pltpu.CompilerParams(
                collective_id=0, has_side_effects=True, vmem_limit_bytes=56 * 1024 * 1024
            ),
        )(image_student, text_student, image_teacher, text_teacher)
        return loss[0, 0], image_grad, text_grad

    return jax.shard_map(
        body,
        mesh=mesh,
        in_specs=(
            P(("row", "col"), None),
            P(("col", "row"), None),
            P(("row", "col"), None),
            P(("col", "row"), None),
        ),
        out_specs=(P(), P(("row", "col"), None), P(("col", "row"), None)),
        check_vma=False,
    )
```

```python
import functools

import jax
import jax.numpy as jnp
from jax import lax
from jax.experimental import pallas as pl
from jax.experimental.pallas import tpu as pltpu
from jax.sharding import PartitionSpec as P

logit_scale = 100.0
MESH = pl.DeviceIdType.MESH
f32, bf16 = jnp.float32, jnp.bfloat16


def layout(mesh_shape):
    rows, cols = mesh_shape["row"], mesh_shape["col"]
    cores = 2 if cols % 2 == 0 else 1
    chips = cols // cores
    divisors = [d for d in range(1, chips + 1) if chips % d == 0]
    a = min(divisors, key=lambda d: d + rows * chips // d)
    q = max(d for d in range(1, a + 1) if a % d == 0 and d * d <= a)
    return dict(R=rows, C=cols, K=cores, A=a, H=chips // a, Q=q, P=a // q)


def contract_last(left, right):
    return lax.dot_general(left, right, (((1,), (1,)), ((), ())), preferred_element_type=f32)


def contract_first(left, right):
    return lax.dot_general(left, right, (((0,), (0,)), ((), ())), preferred_element_type=f32)


def merged(slots, count):
    def line(index, which):
        return slots[index, which : which + 1, :]

    student_high = functools.reduce(jnp.maximum, [line(i, 0) for i in range(count)])
    teacher_high = functools.reduce(jnp.maximum, [line(i, 2) for i in range(count)])
    student_total = teacher_total = divergence = 0.0
    for i in range(count):
        student_total += line(i, 1) * jnp.exp(line(i, 0) - student_high)
        factor = jnp.exp(line(i, 2) - teacher_high)
        teacher_total += line(i, 3) * factor
        divergence += line(i, 4) * factor
    student_lse = student_high + jnp.log(student_total)
    teacher_lse = teacher_high + jnp.log(teacher_total)
    kl = divergence / teacher_total - teacher_lse + student_lse
    return student_lse, teacher_lse, 0.5 * (student_lse + kl)


def position(index, step, count):
    total = jnp.zeros_like(index)
    for t in range(1, count):
        total += (index >= t * step).astype(jnp.int32)
    return total


def kernel(
    g, n_send, total,
    is_hbm, ts_hbm, it_hbm, tt_hbm,
    loss_ref, ig_ref, tg_ref,
    imgs, imgo, imgt, txts, txtt,
    s_ref, t_ref, rowtmp, rstat, cstat, la, lb, gbuf, grecv,
    pi, inarrow, inear, idirect, ijoint, ifar, pt, tnarrow, tnear, tdirect, tjoint, tfar,
    local_sem, send_sem, rimgs, rimgo, rimgt, rtxts, rtxtt, rrow, rcol, rla, rlb, rg,
    rinear, ridirect, rifar, rtnear, rtdirect, rtfar,
):
    R, K, A, H, Q, PP = g["R"], g["K"], g["A"], g["H"], g["Q"], g["P"]
    n, S = is_hbm.shape[0], g["S"]
    m = n // S
    r = lax.axis_index("row")
    c = lax.axis_index("col")
    k, chip = lax.rem(c, K), lax.div(c, K)
    lo, hi = lax.rem(chip, A), lax.div(chip, A)
    q, p = lax.rem(lo, Q), lax.div(lo, Q)
    HR, T = H * R, K * H * R

    def dev(r_, hi_, lo_, k_):
        return (r_, (hi_ * A + lo_) * K + k_)

    def up(value, step, count):
        return lax.rem(value + step, count)

    def down(value, step, count):
        return lax.rem(value + count - step, count)

    def block(ref, index):
        return ref.at[pl.ds(pl.multiple_of(index * n, n), n), :]

    def piece(ref, index, j):
        return ref.at[pl.ds(pl.multiple_of(index * n + j * m, m), m), :]

    a_peers = [dev(r, hi, up(lo, d, A), k) for d in range(1, A)]
    b_steps = [(dk, dh, dr) for dk in range(K) for dh in range(H) for dr in range(R)]
    b_peers = [dev(up(r, dr, R), up(hi, dh, H), lo, up(k, dk, K)) for dk, dh, dr in b_steps[1:]]
    partner = dev(r, hi, lo, up(k, 1, K))

    pending = []

    def send(src, dst, recv, target):
        copy = pltpu.make_async_remote_copy(
            src_ref=src, dst_ref=dst, send_sem=send_sem.at[len(pending)], recv_sem=recv,
            device_id=target, device_id_type=MESH,
        )
        copy.start()
        pending.append(copy)

    def arrived(ref, recv):
        pltpu.make_async_remote_copy(
            src_ref=ref, dst_ref=ref, send_sem=send_sem.at[0], recv_sem=recv,
            device_id=partner, device_id_type=MESH,
        ).wait_recv()

    own_text = (k * H + hi) * R + r
    loads = []
    for i, (src, dst) in enumerate((
        (is_hbm, block(imgs, lo)), (ts_hbm, block(txts, own_text)),
        (it_hbm, block(imgt, lo)), (tt_hbm, block(txtt, own_text)),
    )):
        copy = pltpu.make_async_copy(src, dst, local_sem.at[i])
        copy.start()
        loads.append(copy)
    barrier = pltpu.get_barrier_semaphore()
    for target in a_peers + b_peers:
        pl.semaphore_signal(barrier, inc=1, device_id=target, device_id_type=MESH)
    pl.semaphore_wait(barrier, len(a_peers) + len(b_peers))

    def image_slot(dp, dq):
        return down(p, dp, PP) * Q + down(q, dq, Q)

    def text_slot(dk, dh, dr):
        return (down(k, dk, K) * H + down(hi, dh, H)) * R + down(r, dr, R)

    def text_at(dk, dh, dr):
        return (dk * H + dh) * R + dr

    def image_own(ref, sems, j):
        for dp in range(1, PP):
            send(piece(ref, lo, j), piece(ref, lo, j), sems.at[dp * Q, j],
                 dev(r, hi, up(p, dp, PP) * Q + q, k))

    def image_spread(ref, sems, dp, j):
        slot = image_slot(dp, 0)
        for dq in range(1, Q):
            send(piece(ref, slot, j), piece(ref, slot, j), sems.at[dp * Q + dq, j],
                 dev(r, hi, p * Q + up(q, dq, Q), k))

    def text_own(ref, sems, j):
        for dh in range(1, H):
            send(piece(ref, own_text, j), piece(ref, own_text, j), sems.at[text_at(0, dh, 0), j],
                 dev(r, up(hi, dh, H), lo, k))

    def text_spread(ref, sems, dh, j):
        slot = text_slot(0, dh, 0)
        for dr in range(1, R):
            send(piece(ref, slot, j), piece(ref, slot, j), sems.at[text_at(0, dh, dr), j],
                 dev(up(r, dr, R), hi, lo, k))

    def text_across(ref, sems, dh, dr, j):
        slot = text_slot(0, dh, dr)
        for dk in range(1, K):
            send(piece(ref, slot, j), piece(ref, slot, j), sems.at[text_at(dk, dh, dr), j],
                 dev(r, hi, lo, up(k, dk, K)))

    pairs = ((imgs, rimgs, txts, rtxts), (imgt, rimgt, txtt, rtxtt))
    for i, (img, rimg, txt, rtxt) in enumerate(pairs):
        loads[2 * i].wait()
        loads[2 * i + 1].wait()
        for j in range(S):
            image_own(img, rimg, j)
            text_own(txt, rtxt, j)
        for j in range(S):
            image_spread(img, rimg, 0, j)
            text_spread(txt, rtxt, 0, j)
            text_across(txt, rtxt, 0, 0, j)

    def forward(img, rimg, txt, rtxt):
        for j in range(S):
            for dp in range(1, PP):
                arrived(piece(img, image_slot(dp, 0), j), rimg.at[dp * Q, j])
                image_spread(img, rimg, dp, j)
            for dh in range(1, H):
                arrived(piece(txt, text_slot(0, dh, 0), j), rtxt.at[text_at(0, dh, 0), j])
                text_spread(txt, rtxt, dh, j)
                text_across(txt, rtxt, dh, 0, j)

    def collect(img, rimg, txt, rtxt):
        for dh in range(H):
            for j in range(S):
                for dr in range(1, R):
                    arrived(piece(txt, text_slot(0, dh, dr), j), rtxt.at[text_at(0, dh, dr), j])
                    text_across(txt, rtxt, dh, dr, j)
        for j in range(S):
            for dp in range(PP):
                for dq in range(1, Q):
                    arrived(piece(img, image_slot(dp, dq), j), rimg.at[dp * Q + dq, j])
            for dk, dh, dr in b_steps:
                if dk:
                    arrived(piece(txt, text_slot(dk, dh, dr), j), rtxt.at[text_at(dk, dh, dr), j])

    for pair in pairs:
        forward(*pair)
    collect(*pairs[0])
    s_ref[...] = logit_scale * contract_last(imgs[...], txts[...])
    collect(*pairs[1])
    if K > 1:
        send(imgs, imgo, rimgo, partner)
    t_ref[...] = logit_scale * contract_last(imgt[...], txtt[...])

    rows, width = s_ref.shape
    col_s = jnp.max(s_ref[...], axis=0, keepdims=True)
    col_t = jnp.max(t_ref[...], axis=0, keepdims=True)
    lane = lax.broadcasted_iota(jnp.int32, (n, 128), 1)
    col_id = lax.broadcasted_iota(jnp.int32, (1, width), 1)
    col_slot = position(col_id, n, T)
    slot_k, slot_h = position(col_slot, HR, K), position(col_slot, R, K * H)
    slot_r = col_slot - slot_h * R
    slot_h = slot_h - slot_k * H
    col_id = (((slot_h * A + lo) * K + slot_k) * R + slot_r) * n + col_id - col_slot * n
    row_id = lax.broadcasted_iota(jnp.int32, (n, 1), 0)
    sums = [0.0] * 3
    diagonal = 0.0

    def eye(b):
        base = (r * g["C"] + (hi * A + b) * K + k) * n
        return row_id + base == col_id

    for b in range(A):
        at = slice(b * n, (b + 1) * n)
        s, t = s_ref[at, :], t_ref[at, :]
        gap = t - s
        row_s = jnp.max(s, axis=1, keepdims=True)
        row_t = jnp.max(t, axis=1, keepdims=True)
        row_weight = jnp.exp(t - row_t)
        stats = (
            row_s,
            jnp.sum(jnp.exp(s - row_s), axis=1, keepdims=True),
            row_t,
            jnp.sum(row_weight, axis=1, keepdims=True),
            jnp.sum(row_weight * gap, axis=1, keepdims=True),
        )
        packed = jnp.zeros((n, 128), f32)
        for i, value in enumerate(stats):
            packed = jnp.where(lane == i, value, packed)
        rowtmp[at, :] = packed
        col_weight = jnp.exp(t - col_t)
        parts = (jnp.exp(s - col_s), col_weight, col_weight * gap)
        sums = [old + jnp.sum(new, axis=0, keepdims=True) for old, new in zip(sums, parts)]
        diagonal += jnp.sum(jnp.where(eye(b), s, 0.0), axis=0, keepdims=True)
    line = lax.broadcasted_iota(jnp.int32, (8, width), 0)
    packed = jnp.zeros((8, width), f32)
    for i, value in enumerate((col_s, sums[0], col_t, sums[1], sums[2])):
        packed = jnp.where(line == i, value, packed)
    cstat[0] = packed
    for e, target in enumerate(b_peers, 1):
        send(cstat.at[0], cstat.at[e], rcol.at[e], target)
    rstat[0] = jnp.transpose(rowtmp[...])[:8, :]
    for d, target in enumerate(a_peers, 1):
        send(rstat.at[0], rstat.at[d], rrow.at[d], target)
    for d in range(1, A):
        arrived(rstat.at[d], rrow.at[d])
    row_student, row_teacher, row_terms = merged(rstat, A)
    line = lax.broadcasted_iota(jnp.int32, (128, rows), 0)
    rowtmp[...] = jnp.transpose(jnp.where(line == 0, row_student, row_teacher))
    for e in range(1, T):
        arrived(cstat.at[e], rcol.at[e])
    col_student, col_teacher, col_terms = merged(cstat, T)

    at_row = lax.broadcasted_iota(jnp.int32, (1, rows), 1) - lo * n
    at_col = lax.broadcasted_iota(jnp.int32, (1, width), 1) - own_text * n
    share = (
        jnp.sum(jnp.where((at_row >= 0) & (at_row < n), row_terms, 0.0), axis=1, keepdims=True)
        + jnp.sum(
            jnp.where((at_col >= 0) & (at_col < n), col_terms, 0.0) - diagonal,
            axis=1, keepdims=True,
        )
    )
    la[0] = jnp.broadcast_to(share, (8, 128))
    for d, target in enumerate(a_peers, 1):
        send(la.at[0], la.at[d], rla.at[d], target)

    half = width // K
    for b in range(A):
        at = slice(b * n, (b + 1) * n)
        s, t = s_ref[at, :], t_ref[at, :]
        row_s, row_t = rowtmp[at, 0:1], rowtmp[at, 1:2]
        grad = (
            jnp.exp(s - row_s) + jnp.exp(s - col_student)
            - 0.5 * (jnp.exp(t - row_t) + jnp.exp(t - col_teacher))
            - jnp.where(eye(b), 1.0, 0.0)
        ).astype(bf16)
        for j in range(K):
            gbuf[j, at, :] = grad[:, j * half : (j + 1) * half]
    if K > 1:
        send(gbuf.at[up(k, 1, K)], grecv, rg, partner)

    partial = 0.0
    for j in range(K):
        partial += jnp.dot(gbuf[j], txts[j * half : (j + 1) * half, :], preferred_element_type=f32)
    pi[...] = partial

    def first_hops(part, out_index, in_index, outer, inner, narrow, near, nears, direct, directs, target):
        for j in range(S):
            for do in range(1, outer):
                for di in range(1, inner):
                    e = (do - 1) * (inner - 1) + di - 1
                    to = up(in_index, di, inner)
                    send(piece(part, up(out_index, do, outer) * inner + to, j), piece(near, e, j),
                         nears.at[e, j], target(out_index, to))
        for di in range(1, inner):
            to = up(in_index, di, inner)
            block(narrow, di - 1)[...] = block(part, out_index * inner + to)[...].astype(bf16)
            send(block(narrow, di - 1), block(direct, di - 1), directs.at[di - 1], target(out_index, to))

    def second_hops(part, out_index, in_index, outer, inner, near, nears, joint, far, fars, target, j):
        for do in range(1, outer):
            to = up(out_index, do, outer)
            value = piece(part, to * inner + in_index, j)[...]
            for di in range(1, inner):
                e = (do - 1) * (inner - 1) + di - 1
                arrived(piece(near, e, j), nears.at[e, j])
                value += piece(near, e, j)[...]
            piece(joint, do - 1, j)[...] = value.astype(bf16)
            send(piece(joint, do - 1, j), piece(far, do - 1, j), fars.at[do - 1, j], target(to, in_index))

    def last_sum(part, out_index, in_index, outer, inner, direct, directs, far, fars):
        value = block(part, out_index * inner + in_index)[...]
        for di in range(1, inner):
            arrived(block(direct, di - 1), directs.at[di - 1])
            value += block(direct, di - 1)[...].astype(f32)
        for do in range(1, outer):
            for j in range(S):
                arrived(piece(far, do - 1, j), fars.at[do - 1, j])
            value += block(far, do - 1)[...].astype(f32)
        return logit_scale * value

    def image_target(p_, q_):
        return dev(r, hi, p_ * Q + q_, k)

    def text_target(h_, r_):
        return dev(r_, h_, lo, k)

    first_hops(pi, p, q, PP, Q, inarrow, inear, rinear, idirect, ridirect, image_target)

    if K > 1:
        arrived(imgo, rimgo)
        arrived(grecv, rg)
    partial = contract_first(gbuf[k], imgs[...])
    if K > 1:
        partial += contract_first(grecv[...], imgo[...])
    pt[...] = partial
    first_hops(pt, hi, r, H, R, tnarrow, tnear, rtnear, tdirect, rtdirect, text_target)
    for j in range(S):
        second_hops(pi, p, q, PP, Q, inear, rinear, ijoint, ifar, rifar, image_target, j)
        second_hops(pt, hi, r, H, R, tnear, rtnear, tjoint, tfar, rtfar, text_target, j)
        if j == 0:
            for d in range(1, A):
                arrived(la.at[d], rla.at[d])
            lb[0] = functools.reduce(jnp.add, [la[d] for d in range(A)])
            for e, target in enumerate(b_peers, 1):
                send(lb.at[0], lb.at[e], rlb.at[e], target)

    for e in range(1, T):
        arrived(lb.at[e], rlb.at[e])
    loss_ref[...] = functools.reduce(jnp.add, [lb[e] for e in range(T)]) / total
    ig_ref[...] = last_sum(pi, p, q, PP, Q, idirect, ridirect, ifar, rifar)
    tg_ref[...] = last_sum(pt, hi, r, H, R, tdirect, rtdirect, tfar, rtfar)
    for copy in pending:
        copy.wait_send()
    assert len(pending) == n_send, len(pending)


def solution(mesh):
    g = layout(mesh.shape)
    R, K, A, H, Q, PP = g["R"], g["K"], g["A"], g["H"], g["Q"], g["P"]
    HR, T = H * R, K * H * R
    near = ((PP - 1) * (Q - 1), (H - 1) * (R - 1))

    def body(image_student, text_student, image_teacher, text_teacher):
        n, width = image_student.shape
        rows, cols = A * n, T * n
        total = n * R * g["C"]
        S = g["S"] = 4 if n % 64 == 0 else 1
        gather = S * (2 * (A - 1) + 2 * (HR - 1) + 2 * HR * (K - 1)) + (K - 1)
        n_send = gather + 2 * (A - 1) + 2 * (T - 1) + (K - 1)
        n_send += S * (sum(near) + PP - 1 + H - 1) + Q - 1 + R - 1
        vmem, dma = pltpu.VMEM, pltpu.SemaphoreType.DMA

        def sums(size, near, direct, far):
            near, direct, far = max(near, 1) * n, max(direct, 1) * n, max(far, 1) * n
            return (
                vmem((size, width), f32), vmem((direct, width), bf16), vmem((near, width), f32),
                vmem((direct, width), bf16), vmem((far, width), bf16), vmem((far, width), bf16),
            )

        def arrivals(near, direct, far):
            return dma((max(near, 1), S)), dma((max(direct, 1),)), dma((max(far, 1), S))

        block_out = jax.ShapeDtypeStruct((n, width), f32)
        loss, image_grad, text_grad = pl.pallas_call(
            functools.partial(kernel, g, n_send, total),
            out_shape=(jax.ShapeDtypeStruct((8, 128), f32), block_out, block_out),
            in_specs=[pl.BlockSpec(memory_space=pl.ANY)] * 4,
            out_specs=[pl.BlockSpec(memory_space=pltpu.VMEM)] * 3,
            scratch_shapes=[
                vmem((rows, width), bf16), vmem((rows, width), bf16), vmem((rows, width), bf16),
                vmem((cols, width), bf16), vmem((cols, width), bf16),
                vmem((rows, cols), f32), vmem((rows, cols), f32),
                vmem((rows, 128), f32), vmem((A, 8, rows), f32), vmem((T, 8, cols), f32),
                vmem((A, 8, 128), f32), vmem((T, 8, 128), f32),
                vmem((K, rows, cols // K), bf16), vmem((rows, cols // K), bf16),
                *sums(rows, near[0], Q - 1, PP - 1), *sums(cols // K, near[1], R - 1, H - 1),
                dma((4,)), dma((n_send,)),
                dma((A, S)), dma(()), dma((A, S)), dma((T, S)), dma((T, S)),
                dma((A,)), dma((T,)), dma((A,)), dma((T,)), dma(()),
                *arrivals(near[0], Q - 1, PP - 1), *arrivals(near[1], R - 1, H - 1),
            ],
            compiler_params=pltpu.CompilerParams(
                collective_id=0, has_side_effects=True, vmem_limit_bytes=56 * 1024 * 1024
            ),
        )(image_student, text_student, image_teacher, text_teacher)
        return loss[0, 0], image_grad, text_grad

    return jax.shard_map(
        body,
        mesh=mesh,
        in_specs=(
            P(("row", "col"), None),
            P(("col", "row"), None),
            P(("row", "col"), None),
            P(("col", "row"), None),
        ),
        out_specs=(P(), P(("row", "col"), None), P(("col", "row"), None)),
        check_vma=False,
    )
```

```python
import functools

import jax
import jax.numpy as jnp
from jax import lax
from jax.experimental import pallas as pl
from jax.experimental.pallas import tpu as pltpu
from jax.sharding import PartitionSpec as P

logit_scale = 100.0
MESH = pl.DeviceIdType.MESH
f32, bf16 = jnp.float32, jnp.bfloat16


def layout(mesh_shape):
    rows, cols = mesh_shape["row"], mesh_shape["col"]
    cores = 2 if cols % 2 == 0 else 1
    chips = cols // cores
    divisors = [d for d in range(1, chips + 1) if chips % d == 0]
    a = min(divisors, key=lambda d: d + rows * chips // d)
    q = max(d for d in range(1, a + 1) if a % d == 0 and d * d <= a)
    return dict(R=rows, C=cols, K=cores, A=a, H=chips // a, Q=q, P=a // q)


def contract_last(left, right):
    return lax.dot_general(left, right, (((1,), (1,)), ((), ())), preferred_element_type=f32)


def contract_first(left, right):
    return lax.dot_general(left, right, (((0,), (0,)), ((), ())), preferred_element_type=f32)


def merged(slots, count):
    def line(index, which):
        return slots[index, which : which + 1, :]

    student_high = functools.reduce(jnp.maximum, [line(i, 0) for i in range(count)])
    teacher_high = functools.reduce(jnp.maximum, [line(i, 2) for i in range(count)])
    student_total = teacher_total = divergence = 0.0
    for i in range(count):
        student_total += line(i, 1) * jnp.exp(line(i, 0) - student_high)
        factor = jnp.exp(line(i, 2) - teacher_high)
        teacher_total += line(i, 3) * factor
        divergence += line(i, 4) * factor
    student_lse = student_high + jnp.log(student_total)
    teacher_lse = teacher_high + jnp.log(teacher_total)
    kl = divergence / teacher_total - teacher_lse + student_lse
    return student_lse, teacher_lse, 0.5 * (student_lse + kl)


def position(index, step, count):
    total = jnp.zeros_like(index)
    for t in range(1, count):
        total += (index >= t * step).astype(jnp.int32)
    return total


def kernel(
    g, n_send, total,
    is_hbm, ts_hbm, it_hbm, tt_hbm,
    loss_ref, ig_ref, tg_ref,
    imgs, imgo, imgt, txts, txtt,
    s_ref, t_ref, rowtmp, rstat, cstat, la, lb, gbuf, grecv,
    pi, inarrow, inear, islim, islims, idirect, ijoint, ifar,
    pt, tnarrow, tnear, tslim, tslims, tdirect, tjoint, tfar,
    local_sem, send_sem, rimgs, rimgo, rimgt, rtxts, rtxtt, rrow, rcol, rla, rlb, rg,
    rinear, ridirect, rifar, rtnear, rtdirect, rtfar,
):
    R, K, A, H, Q, PP = g["R"], g["K"], g["A"], g["H"], g["Q"], g["P"]
    n, S = is_hbm.shape[0], g["S"]
    m = n // S
    r = lax.axis_index("row")
    c = lax.axis_index("col")
    k, chip = lax.rem(c, K), lax.div(c, K)
    lo, hi = lax.rem(chip, A), lax.div(chip, A)
    q, p = lax.rem(lo, Q), lax.div(lo, Q)
    HR, T = H * R, K * H * R

    def dev(r_, hi_, lo_, k_):
        return (r_, (hi_ * A + lo_) * K + k_)

    def up(value, step, count):
        return lax.rem(value + step, count)

    def down(value, step, count):
        return lax.rem(value + count - step, count)

    def block(ref, index):
        return ref.at[pl.ds(pl.multiple_of(index * n, n), n), :]

    def piece(ref, index, j):
        return ref.at[pl.ds(pl.multiple_of(index * n + j * m, m), m), :]

    a_peers = [dev(r, hi, up(lo, d, A), k) for d in range(1, A)]
    b_steps = [(dk, dh, dr) for dk in range(K) for dh in range(H) for dr in range(R)]
    b_peers = [dev(up(r, dr, R), up(hi, dh, H), lo, up(k, dk, K)) for dk, dh, dr in b_steps[1:]]
    partner = dev(r, hi, lo, up(k, 1, K))

    pending = []

    def send(src, dst, recv, target):
        copy = pltpu.make_async_remote_copy(
            src_ref=src, dst_ref=dst, send_sem=send_sem.at[len(pending)], recv_sem=recv,
            device_id=target, device_id_type=MESH,
        )
        copy.start()
        pending.append(copy)

    def arrived(ref, recv):
        pltpu.make_async_remote_copy(
            src_ref=ref, dst_ref=ref, send_sem=send_sem.at[0], recv_sem=recv,
            device_id=partner, device_id_type=MESH,
        ).wait_recv()

    own_text = (k * H + hi) * R + r
    loads = []
    for i, (src, dst) in enumerate((
        (is_hbm, block(imgs, lo)), (ts_hbm, block(txts, own_text)),
        (it_hbm, block(imgt, lo)), (tt_hbm, block(txtt, own_text)),
    )):
        copy = pltpu.make_async_copy(src, dst, local_sem.at[i])
        copy.start()
        loads.append(copy)
    barrier = pltpu.get_barrier_semaphore()
    for target in a_peers + b_peers:
        pl.semaphore_signal(barrier, inc=1, device_id=target, device_id_type=MESH)
    pl.semaphore_wait(barrier, len(a_peers) + len(b_peers))

    def image_slot(dp, dq):
        return down(p, dp, PP) * Q + down(q, dq, Q)

    def text_slot(dk, dh, dr):
        return (down(k, dk, K) * H + down(hi, dh, H)) * R + down(r, dr, R)

    def text_at(dk, dh, dr):
        return (dk * H + dh) * R + dr

    def image_own(ref, sems, j):
        for dp in range(1, PP):
            send(piece(ref, lo, j), piece(ref, lo, j), sems.at[dp * Q, j],
                 dev(r, hi, up(p, dp, PP) * Q + q, k))

    def image_spread(ref, sems, dp, j):
        slot = image_slot(dp, 0)
        for dq in range(1, Q):
            send(piece(ref, slot, j), piece(ref, slot, j), sems.at[dp * Q + dq, j],
                 dev(r, hi, p * Q + up(q, dq, Q), k))

    def text_own(ref, sems, j):
        for dh in range(1, H):
            send(piece(ref, own_text, j), piece(ref, own_text, j), sems.at[text_at(0, dh, 0), j],
                 dev(r, up(hi, dh, H), lo, k))

    def text_spread(ref, sems, dh, j):
        slot = text_slot(0, dh, 0)
        for dr in range(1, R):
            send(piece(ref, slot, j), piece(ref, slot, j), sems.at[text_at(0, dh, dr), j],
                 dev(up(r, dr, R), hi, lo, k))

    def text_across(ref, sems, dh, dr, j):
        slot = text_slot(0, dh, dr)
        for dk in range(1, K):
            send(piece(ref, slot, j), piece(ref, slot, j), sems.at[text_at(dk, dh, dr), j],
                 dev(r, hi, lo, up(k, dk, K)))

    pairs = ((imgs, rimgs, txts, rtxts), (imgt, rimgt, txtt, rtxtt))
    for i, (img, rimg, txt, rtxt) in enumerate(pairs):
        loads[2 * i].wait()
        loads[2 * i + 1].wait()
        for j in range(S):
            image_own(img, rimg, j)
            text_own(txt, rtxt, j)
        for j in range(S):
            image_spread(img, rimg, 0, j)
            text_spread(txt, rtxt, 0, j)
            text_across(txt, rtxt, 0, 0, j)

    def forward(img, rimg, txt, rtxt):
        for j in range(S):
            for dp in range(1, PP):
                arrived(piece(img, image_slot(dp, 0), j), rimg.at[dp * Q, j])
                image_spread(img, rimg, dp, j)
            for dh in range(1, H):
                arrived(piece(txt, text_slot(0, dh, 0), j), rtxt.at[text_at(0, dh, 0), j])
                text_spread(txt, rtxt, dh, j)
                text_across(txt, rtxt, dh, 0, j)

    def collect(img, rimg, txt, rtxt):
        for dh in range(H):
            for j in range(S):
                for dr in range(1, R):
                    arrived(piece(txt, text_slot(0, dh, dr), j), rtxt.at[text_at(0, dh, dr), j])
                    text_across(txt, rtxt, dh, dr, j)
        for j in range(S):
            for dp in range(PP):
                for dq in range(1, Q):
                    arrived(piece(img, image_slot(dp, dq), j), rimg.at[dp * Q + dq, j])
            for dk, dh, dr in b_steps:
                if dk:
                    arrived(piece(txt, text_slot(dk, dh, dr), j), rtxt.at[text_at(dk, dh, dr), j])

    for pair in pairs:
        forward(*pair)
    collect(*pairs[0])
    s_ref[...] = logit_scale * contract_last(imgs[...], txts[...])
    rows, width = s_ref.shape
    lane = lax.broadcasted_iota(jnp.int32, (n, 128), 1)
    col_id = lax.broadcasted_iota(jnp.int32, (1, width), 1)
    col_slot = position(col_id, n, T)
    slot_k, slot_h = position(col_slot, HR, K), position(col_slot, R, K * H)
    slot_r = col_slot - slot_h * R
    slot_h = slot_h - slot_k * H
    col_id = (((slot_h * A + lo) * K + slot_k) * R + slot_r) * n + col_id - col_slot * n
    row_id = lax.broadcasted_iota(jnp.int32, (n, 1), 0)

    def eye(b):
        base = (r * g["C"] + (hi * A + b) * K + k) * n
        return row_id + base == col_id

    def pack(values, into, index):
        for i, value in values:
            into = jnp.where(index == i, value, into)
        return into

    col_s = jnp.max(s_ref[...], axis=0, keepdims=True)
    col_total = diagonal = 0.0
    for b in range(A):
        at = slice(b * n, (b + 1) * n)
        s = s_ref[at, :]
        row_s = jnp.max(s, axis=1, keepdims=True)
        row_total = jnp.sum(jnp.exp(s - row_s), axis=1, keepdims=True)
        rowtmp[at, :] = pack(((0, row_s), (1, row_total)), jnp.zeros((n, 128), f32), lane)
        col_total += jnp.sum(jnp.exp(s - col_s), axis=0, keepdims=True)
        diagonal += jnp.sum(jnp.where(eye(b), s, 0.0), axis=0, keepdims=True)
    collect(*pairs[1])
    if K > 1:
        send(imgs, imgo, rimgo, partner)
    t_ref[...] = logit_scale * contract_last(imgt[...], txtt[...])

    col_t = jnp.max(t_ref[...], axis=0, keepdims=True)
    sums = [0.0] * 2
    for b in range(A):
        at = slice(b * n, (b + 1) * n)
        s, t = s_ref[at, :], t_ref[at, :]
        gap = t - s
        row_t = jnp.max(t, axis=1, keepdims=True)
        row_weight = jnp.exp(t - row_t)
        row_sums = [jnp.sum(v, axis=1, keepdims=True) for v in (row_weight, row_weight * gap)]
        rowtmp[at, :] = pack(((2, row_t), (3, row_sums[0]), (4, row_sums[1])), rowtmp[at, :], lane)
        col_weight = jnp.exp(t - col_t)
        sums = [
            old + jnp.sum(new, axis=0, keepdims=True)
            for old, new in zip(sums, (col_weight, col_weight * gap))
        ]
    line = lax.broadcasted_iota(jnp.int32, (8, width), 0)
    packed = pack(enumerate((col_s, col_total, col_t, *sums)), jnp.zeros((8, width), f32), line)
    cstat[0] = packed
    for e, target in enumerate(b_peers, 1):
        send(cstat.at[0], cstat.at[e], rcol.at[e], target)
    rstat[0] = jnp.transpose(rowtmp[...])[:8, :]
    for d, target in enumerate(a_peers, 1):
        send(rstat.at[0], rstat.at[d], rrow.at[d], target)
    for d in range(1, A):
        arrived(rstat.at[d], rrow.at[d])
    row_student, row_teacher, row_terms = merged(rstat, A)
    line = lax.broadcasted_iota(jnp.int32, (128, rows), 0)
    rowtmp[...] = jnp.transpose(jnp.where(line == 0, row_student, row_teacher))
    for e in range(1, T):
        arrived(cstat.at[e], rcol.at[e])
    col_student, col_teacher, col_terms = merged(cstat, T)

    at_row = lax.broadcasted_iota(jnp.int32, (1, rows), 1) - lo * n
    at_col = lax.broadcasted_iota(jnp.int32, (1, width), 1) - own_text * n
    share = (
        jnp.sum(jnp.where((at_row >= 0) & (at_row < n), row_terms, 0.0), axis=1, keepdims=True)
        + jnp.sum(
            jnp.where((at_col >= 0) & (at_col < n), col_terms, 0.0) - diagonal,
            axis=1, keepdims=True,
        )
    )
    la[0] = jnp.broadcast_to(share, (8, 128))
    for d, target in enumerate(a_peers, 1):
        send(la.at[0], la.at[d], rla.at[d], target)

    half = width // K
    for b in range(A):
        at = slice(b * n, (b + 1) * n)
        s, t = s_ref[at, :], t_ref[at, :]
        row_s, row_t = rowtmp[at, 0:1], rowtmp[at, 1:2]
        grad = (
            jnp.exp(s - row_s) + jnp.exp(s - col_student)
            - 0.5 * (jnp.exp(t - row_t) + jnp.exp(t - col_teacher))
            - jnp.where(eye(b), 1.0, 0.0)
        ).astype(bf16)
        for j in range(K):
            gbuf[j, at, :] = grad[:, j * half : (j + 1) * half]
    if K > 1:
        send(gbuf.at[up(k, 1, K)], grecv, rg, partner)

    partial = 0.0
    for j in range(K):
        partial += jnp.dot(gbuf[j], txts[j * half : (j + 1) * half, :], preferred_element_type=f32)
    pi[...] = partial

    def first_hops(part, out_index, in_index, outer, inner, narrow, near, nears, slim, slims, direct, directs, target):
        for j in range(S):
            for do in range(1, outer):
                for di in range(1, inner):
                    e = (do - 1) * (inner - 1) + di - 1
                    to = up(in_index, di, inner)
                    src = piece(part, up(out_index, do, outer) * inner + to, j)
                    if j % 2 == 0:
                        piece(slims, e, j)[...] = src[...].astype(bf16)
                        send(piece(slims, e, j), piece(slim, e, j), nears.at[e, j], target(out_index, to))
                    else:
                        send(src, piece(near, e, j), nears.at[e, j], target(out_index, to))
        for di in range(1, inner):
            to = up(in_index, di, inner)
            block(narrow, di - 1)[...] = block(part, out_index * inner + to)[...].astype(bf16)
            send(block(narrow, di - 1), block(direct, di - 1), directs.at[di - 1], target(out_index, to))

    def second_hops(part, out_index, in_index, outer, inner, near, nears, slim, joint, far, fars, target, j):
        for do in range(1, outer):
            to = up(out_index, do, outer)
            value = piece(part, to * inner + in_index, j)[...]
            for di in range(1, inner):
                e = (do - 1) * (inner - 1) + di - 1
                landed = piece(slim if j % 2 == 0 else near, e, j)
                arrived(landed, nears.at[e, j])
                value += landed[...].astype(f32)
            piece(joint, do - 1, j)[...] = value.astype(bf16)
            send(piece(joint, do - 1, j), piece(far, do - 1, j), fars.at[do - 1, j], target(to, in_index))

    def last_sum(part, out_index, in_index, outer, inner, direct, directs, far, fars):
        value = block(part, out_index * inner + in_index)[...]
        for di in range(1, inner):
            arrived(block(direct, di - 1), directs.at[di - 1])
            value += block(direct, di - 1)[...].astype(f32)
        for do in range(1, outer):
            for j in range(S):
                arrived(piece(far, do - 1, j), fars.at[do - 1, j])
            value += block(far, do - 1)[...].astype(f32)
        return logit_scale * value

    def image_target(p_, q_):
        return dev(r, hi, p_ * Q + q_, k)

    def text_target(h_, r_):
        return dev(r_, h_, lo, k)

    first_hops(pi, p, q, PP, Q, inarrow, inear, rinear, islim, islims, idirect, ridirect, image_target)

    if K > 1:
        arrived(imgo, rimgo)
        arrived(grecv, rg)
    partial = contract_first(gbuf[k], imgs[...])
    if K > 1:
        partial += contract_first(grecv[...], imgo[...])
    pt[...] = partial
    first_hops(pt, hi, r, H, R, tnarrow, tnear, rtnear, tslim, tslims, tdirect, rtdirect, text_target)
    for j in range(S):
        second_hops(pi, p, q, PP, Q, inear, rinear, islim, ijoint, ifar, rifar, image_target, j)
        second_hops(pt, hi, r, H, R, tnear, rtnear, tslim, tjoint, tfar, rtfar, text_target, j)
        if j == 0:
            for d in range(1, A):
                arrived(la.at[d], rla.at[d])
            lb[0] = functools.reduce(jnp.add, [la[d] for d in range(A)])
            for e, target in enumerate(b_peers, 1):
                send(lb.at[0], lb.at[e], rlb.at[e], target)

    for e in range(1, T):
        arrived(lb.at[e], rlb.at[e])
    loss_ref[...] = functools.reduce(jnp.add, [lb[e] for e in range(T)]) / total
    ig_ref[...] = last_sum(pi, p, q, PP, Q, idirect, ridirect, ifar, rifar)
    tg_ref[...] = last_sum(pt, hi, r, H, R, tdirect, rtdirect, tfar, rtfar)
    for copy in pending:
        copy.wait_send()
    assert len(pending) == n_send, len(pending)


def leave(loss_in, image_in, text_in, loss_out, image_out, text_out, sems):
    image_copy = pltpu.make_async_copy(image_in, image_out, sems.at[0])
    text_copy = pltpu.make_async_copy(text_in, text_out, sems.at[1])
    image_copy.start()
    text_copy.start()
    loss_out[0, 0] = jnp.max(loss_in[...])
    image_copy.wait()
    text_copy.wait()


def solution(mesh):
    g = layout(mesh.shape)
    R, K, A, H, Q, PP = g["R"], g["K"], g["A"], g["H"], g["Q"], g["P"]
    HR, T = H * R, K * H * R
    near = ((PP - 1) * (Q - 1), (H - 1) * (R - 1))

    def body(image_student, text_student, image_teacher, text_teacher):
        n, width = image_student.shape
        rows, cols = A * n, T * n
        total = n * R * g["C"]
        S = g["S"] = 4 if n % 64 == 0 else 1
        gather = S * (2 * (A - 1) + 2 * (HR - 1) + 2 * HR * (K - 1)) + (K - 1)
        n_send = gather + 2 * (A - 1) + 2 * (T - 1) + (K - 1)
        n_send += S * (sum(near) + PP - 1 + H - 1) + Q - 1 + R - 1
        vmem, dma = pltpu.VMEM, pltpu.SemaphoreType.DMA

        def sums(size, near, direct, far):
            near, direct, far = max(near, 1) * n, max(direct, 1) * n, max(far, 1) * n
            return (
                vmem((size, width), f32), vmem((direct, width), bf16), vmem((near, width), f32),
                vmem((near, width), bf16), vmem((near, width), bf16),
                vmem((direct, width), bf16), vmem((far, width), bf16), vmem((far, width), bf16),
            )

        def arrivals(near, direct, far):
            return dma((max(near, 1), S)), dma((max(direct, 1),)), dma((max(far, 1), S))

        block_out = jax.ShapeDtypeStruct((n, width), f32)
        loss, image_grad, text_grad = pl.pallas_call(
            functools.partial(kernel, g, n_send, total),
            out_shape=(vmem((8, 128), f32), vmem((n, width), f32), vmem((n, width), f32)),
            in_specs=[pl.BlockSpec(memory_space=pl.ANY)] * 4,
            out_specs=[pl.BlockSpec(memory_space=pltpu.VMEM)] * 3,
            scratch_shapes=[
                vmem((rows, width), bf16), vmem((rows, width), bf16), vmem((rows, width), bf16),
                vmem((cols, width), bf16), vmem((cols, width), bf16),
                vmem((rows, cols), f32), vmem((rows, cols), f32),
                vmem((rows, 128), f32), vmem((A, 8, rows), f32), vmem((T, 8, cols), f32),
                vmem((A, 8, 128), f32), vmem((T, 8, 128), f32),
                vmem((K, rows, cols // K), bf16), vmem((rows, cols // K), bf16),
                *sums(rows, near[0], Q - 1, PP - 1), *sums(cols // K, near[1], R - 1, H - 1),
                dma((4,)), dma((n_send,)),
                dma((A, S)), dma(()), dma((A, S)), dma((T, S)), dma((T, S)),
                dma((A,)), dma((T,)), dma((A,)), dma((T,)), dma(()),
                *arrivals(near[0], Q - 1, PP - 1), *arrivals(near[1], R - 1, H - 1),
            ],
            compiler_params=pltpu.CompilerParams(
                collective_id=0, has_side_effects=True, vmem_limit_bytes=56 * 1024 * 1024
            ),
        )(image_student, text_student, image_teacher, text_teacher)
        loss, image_grad, text_grad = pl.pallas_call(
            leave,
            out_shape=(jax.ShapeDtypeStruct((1, 1), f32), block_out, block_out),
            in_specs=[pl.BlockSpec(memory_space=pltpu.VMEM)] * 3,
            out_specs=[pl.BlockSpec(memory_space=pltpu.SMEM)] + [pl.BlockSpec(memory_space=pl.ANY)] * 2,
            scratch_shapes=[dma((2,))],
            compiler_params=pltpu.CompilerParams(vmem_limit_bytes=1024 * 1024),
        )(loss, image_grad, text_grad)
        return loss[0, 0], image_grad, text_grad

    return jax.shard_map(
        body,
        mesh=mesh,
        in_specs=(
            P(("row", "col"), None),
            P(("col", "row"), None),
            P(("row", "col"), None),
            P(("col", "row"), None),
        ),
        out_specs=(P(), P(("row", "col"), None), P(("col", "row"), None)),
        check_vma=False,
    )
```

```python
import functools

import jax
import jax.numpy as jnp
from jax import lax
from jax.experimental import pallas as pl
from jax.experimental.pallas import tpu as pltpu
from jax.sharding import PartitionSpec as P

logit_scale = 100.0
MESH = pl.DeviceIdType.MESH
f32, bf16 = jnp.float32, jnp.bfloat16


def layout(mesh_shape):
    rows, cols = mesh_shape["row"], mesh_shape["col"]
    cores = 2 if cols % 2 == 0 else 1
    chips = cols // cores
    divisors = [d for d in range(1, chips + 1) if chips % d == 0]
    a = min(divisors, key=lambda d: d + rows * chips // d)
    q = max(d for d in range(1, a + 1) if a % d == 0 and d * d <= a)
    return dict(R=rows, C=cols, K=cores, A=a, H=chips // a, Q=q, P=a // q)


def contract_last(left, right):
    return lax.dot_general(left, right, (((1,), (1,)), ((), ())), preferred_element_type=f32)


def contract_first(left, right):
    return lax.dot_general(left, right, (((0,), (0,)), ((), ())), preferred_element_type=f32)


def merged(slots, count):
    def line(index, which):
        return slots[index, which : which + 1, :]

    student_high = functools.reduce(jnp.maximum, [line(i, 0) for i in range(count)])
    teacher_high = functools.reduce(jnp.maximum, [line(i, 2) for i in range(count)])
    student_total = teacher_total = divergence = 0.0
    for i in range(count):
        student_total += line(i, 1) * jnp.exp(line(i, 0) - student_high)
        factor = jnp.exp(line(i, 2) - teacher_high)
        teacher_total += line(i, 3) * factor
        divergence += line(i, 4) * factor
    student_lse = student_high + jnp.log(student_total)
    teacher_lse = teacher_high + jnp.log(teacher_total)
    kl = divergence / teacher_total - teacher_lse + student_lse
    return student_lse, teacher_lse, 0.5 * (student_lse + kl)


def position(index, step, count):
    total = jnp.zeros_like(index)
    for t in range(1, count):
        total += (index >= t * step).astype(jnp.int32)
    return total


def kernel(
    g, n_send, total,
    is_hbm, ts_hbm, it_hbm, tt_hbm,
    loss_ref, ig_ref, tg_ref,
    imgs, imgo, imgt, txts, txtt,
    s_ref, t_ref, rowtmp, rstat, cstat, la, lb, gbuf, grecv,
    pi, inarrow, inear, islim, islims, idirect, ijoint, ifar,
    pt, tnarrow, tnear, tslim, tslims, tdirect, tjoint, tfar,
    local_sem, send_sem, rimgs, rimgo, rimgt, rtxts, rtxtt, rrow, rcol, rla, rlb, rg,
    rinear, ridirect, rifar, rtnear, rtdirect, rtfar,
):
    R, K, A, H, Q, PP = g["R"], g["K"], g["A"], g["H"], g["Q"], g["P"]
    n, S = is_hbm.shape[0], g["S"]
    m = n // S
    r = lax.axis_index("row")
    c = lax.axis_index("col")
    k, chip = lax.rem(c, K), lax.div(c, K)
    lo, hi = lax.rem(chip, A), lax.div(chip, A)
    q, p = lax.rem(lo, Q), lax.div(lo, Q)
    HR, T = H * R, K * H * R

    def dev(r_, hi_, lo_, k_):
        return (r_, (hi_ * A + lo_) * K + k_)

    def up(value, step, count):
        return lax.rem(value + step, count)

    def down(value, step, count):
        return lax.rem(value + count - step, count)

    def block(ref, index):
        return ref.at[pl.ds(pl.multiple_of(index * n, n), n), :]

    def piece(ref, index, j):
        return ref.at[pl.ds(pl.multiple_of(index * n + j * m, m), m), :]

    a_peers = [dev(r, hi, up(lo, d, A), k) for d in range(1, A)]
    b_steps = [(dk, dh, dr) for dk in range(K) for dh in range(H) for dr in range(R)]
    b_peers = [dev(up(r, dr, R), up(hi, dh, H), lo, up(k, dk, K)) for dk, dh, dr in b_steps[1:]]
    partner = dev(r, hi, lo, up(k, 1, K))

    pending = []

    def send(src, dst, recv, target):
        copy = pltpu.make_async_remote_copy(
            src_ref=src, dst_ref=dst, send_sem=send_sem.at[len(pending)], recv_sem=recv,
            device_id=target, device_id_type=MESH,
        )
        copy.start()
        pending.append(copy)

    def arrived(ref, recv):
        pltpu.make_async_remote_copy(
            src_ref=ref, dst_ref=ref, send_sem=send_sem.at[0], recv_sem=recv,
            device_id=partner, device_id_type=MESH,
        ).wait_recv()

    own_text = (k * H + hi) * R + r
    loads = []
    for i, (src, dst) in enumerate((
        (is_hbm, block(imgs, lo)), (ts_hbm, block(txts, own_text)),
        (it_hbm, block(imgt, lo)), (tt_hbm, block(txtt, own_text)),
    )):
        copy = pltpu.make_async_copy(src, dst, local_sem.at[i])
        copy.start()
        loads.append(copy)
    barrier = pltpu.get_barrier_semaphore()
    for target in a_peers + b_peers:
        pl.semaphore_signal(barrier, inc=1, device_id=target, device_id_type=MESH)
    pl.semaphore_wait(barrier, len(a_peers) + len(b_peers))

    def image_slot(dp, dq):
        return down(p, dp, PP) * Q + down(q, dq, Q)

    def text_slot(dk, dh, dr):
        return (down(k, dk, K) * H + down(hi, dh, H)) * R + down(r, dr, R)

    def text_at(dk, dh, dr):
        return (dk * H + dh) * R + dr

    def image_own(ref, sems, j):
        for dp in range(1, PP):
            send(piece(ref, lo, j), piece(ref, lo, j), sems.at[dp * Q, j],
                 dev(r, hi, up(p, dp, PP) * Q + q, k))

    def image_spread(ref, sems, dp, j):
        slot = image_slot(dp, 0)
        for dq in range(1, Q):
            send(piece(ref, slot, j), piece(ref, slot, j), sems.at[dp * Q + dq, j],
                 dev(r, hi, p * Q + up(q, dq, Q), k))

    def text_own(ref, sems, j):
        for dh in range(1, H):
            send(piece(ref, own_text, j), piece(ref, own_text, j), sems.at[text_at(0, dh, 0), j],
                 dev(r, up(hi, dh, H), lo, k))

    def text_spread(ref, sems, dh, j):
        slot = text_slot(0, dh, 0)
        for dr in range(1, R):
            send(piece(ref, slot, j), piece(ref, slot, j), sems.at[text_at(0, dh, dr), j],
                 dev(up(r, dr, R), hi, lo, k))

    def text_across(ref, sems, dh, dr, j):
        slot = text_slot(0, dh, dr)
        for dk in range(1, K):
            send(piece(ref, slot, j), piece(ref, slot, j), sems.at[text_at(dk, dh, dr), j],
                 dev(r, hi, lo, up(k, dk, K)))

    pairs = ((imgs, rimgs, txts, rtxts), (imgt, rimgt, txtt, rtxtt))
    for i, (img, rimg, txt, rtxt) in enumerate(pairs):
        loads[2 * i].wait()
        loads[2 * i + 1].wait()
        for j in range(S):
            image_own(img, rimg, j)
            text_own(txt, rtxt, j)
        for j in range(S):
            image_spread(img, rimg, 0, j)
            text_spread(txt, rtxt, 0, j)
            text_across(txt, rtxt, 0, 0, j)

    def forward(img, rimg, txt, rtxt):
        for j in range(S):
            for dp in range(1, PP):
                arrived(piece(img, image_slot(dp, 0), j), rimg.at[dp * Q, j])
                image_spread(img, rimg, dp, j)
            for dh in range(1, H):
                arrived(piece(txt, text_slot(0, dh, 0), j), rtxt.at[text_at(0, dh, 0), j])
                text_spread(txt, rtxt, dh, j)
                text_across(txt, rtxt, dh, 0, j)

    def collect(img, rimg, txt, rtxt):
        for dh in range(H):
            for j in range(S):
                for dr in range(1, R):
                    arrived(piece(txt, text_slot(0, dh, dr), j), rtxt.at[text_at(0, dh, dr), j])
                    text_across(txt, rtxt, dh, dr, j)
        for j in range(S):
            for dp in range(PP):
                for dq in range(1, Q):
                    arrived(piece(img, image_slot(dp, dq), j), rimg.at[dp * Q + dq, j])
            for dk, dh, dr in b_steps:
                if dk:
                    arrived(piece(txt, text_slot(dk, dh, dr), j), rtxt.at[text_at(dk, dh, dr), j])

    for pair in pairs:
        forward(*pair)
    collect(*pairs[0])
    s_ref[...] = logit_scale * contract_last(imgs[...], txts[...])
    rows, width = s_ref.shape
    lane = lax.broadcasted_iota(jnp.int32, (n, 128), 1)
    col_id = lax.broadcasted_iota(jnp.int32, (1, width), 1)
    col_slot = position(col_id, n, T)
    slot_k, slot_h = position(col_slot, HR, K), position(col_slot, R, K * H)
    slot_r = col_slot - slot_h * R
    slot_h = slot_h - slot_k * H
    col_id = (((slot_h * A + lo) * K + slot_k) * R + slot_r) * n + col_id - col_slot * n
    row_id = lax.broadcasted_iota(jnp.int32, (n, 1), 0)

    def eye(b):
        base = (r * g["C"] + (hi * A + b) * K + k) * n
        return row_id + base == col_id

    def pack(values, into, index):
        for i, value in values:
            into = jnp.where(index == i, value, into)
        return into

    col_s = jnp.max(s_ref[...], axis=0, keepdims=True)
    col_total = diagonal = 0.0
    for b in range(A):
        at = slice(b * n, (b + 1) * n)
        s = s_ref[at, :]
        row_s = jnp.max(s, axis=1, keepdims=True)
        row_total = jnp.sum(jnp.exp(s - row_s), axis=1, keepdims=True)
        rowtmp[at, :] = pack(((0, row_s), (1, row_total)), jnp.zeros((n, 128), f32), lane)
        col_total += jnp.sum(jnp.exp(s - col_s), axis=0, keepdims=True)
        diagonal += jnp.sum(jnp.where(eye(b), s, 0.0), axis=0, keepdims=True)
    collect(*pairs[1])
    if K > 1:
        send(imgs, imgo, rimgo, partner)
    t_ref[...] = logit_scale * contract_last(imgt[...], txtt[...])

    col_t = jnp.max(t_ref[...], axis=0, keepdims=True)
    sums = [0.0] * 2
    for b in range(A):
        at = slice(b * n, (b + 1) * n)
        s, t = s_ref[at, :], t_ref[at, :]
        gap = t - s
        row_t = jnp.max(t, axis=1, keepdims=True)
        row_weight = jnp.exp(t - row_t)
        row_sums = [jnp.sum(v, axis=1, keepdims=True) for v in (row_weight, row_weight * gap)]
        rowtmp[at, :] = pack(((2, row_t), (3, row_sums[0]), (4, row_sums[1])), rowtmp[at, :], lane)
        col_weight = jnp.exp(t - col_t)
        sums = [
            old + jnp.sum(new, axis=0, keepdims=True)
            for old, new in zip(sums, (col_weight, col_weight * gap))
        ]
    line = lax.broadcasted_iota(jnp.int32, (8, width), 0)
    packed = pack(enumerate((col_s, col_total, col_t, *sums)), jnp.zeros((8, width), f32), line)
    cstat[0] = packed
    for e, target in enumerate(b_peers, 1):
        send(cstat.at[0], cstat.at[e], rcol.at[e], target)
    rstat[0] = jnp.transpose(rowtmp[...])[:8, :]
    for d, target in enumerate(a_peers, 1):
        send(rstat.at[0], rstat.at[d], rrow.at[d], target)
    for d in range(1, A):
        arrived(rstat.at[d], rrow.at[d])
    row_student, row_teacher, row_terms = merged(rstat, A)
    line = lax.broadcasted_iota(jnp.int32, (128, rows), 0)
    rowtmp[...] = jnp.transpose(jnp.where(line == 0, row_student, row_teacher))
    for e in range(1, T):
        arrived(cstat.at[e], rcol.at[e])
    col_student, col_teacher, col_terms = merged(cstat, T)

    at_row = lax.broadcasted_iota(jnp.int32, (1, rows), 1) - lo * n
    at_col = lax.broadcasted_iota(jnp.int32, (1, width), 1) - own_text * n
    share = (
        jnp.sum(jnp.where((at_row >= 0) & (at_row < n), row_terms, 0.0), axis=1, keepdims=True)
        + jnp.sum(
            jnp.where((at_col >= 0) & (at_col < n), col_terms, 0.0) - diagonal,
            axis=1, keepdims=True,
        )
    )
    la[0] = jnp.broadcast_to(share, (8, 128))
    for d, target in enumerate(a_peers, 1):
        send(la.at[0], la.at[d], rla.at[d], target)

    half = width // K
    for b in range(A):
        at = slice(b * n, (b + 1) * n)
        s, t = s_ref[at, :], t_ref[at, :]
        row_s, row_t = rowtmp[at, 0:1], rowtmp[at, 1:2]
        grad = (
            jnp.exp(s - row_s) + jnp.exp(s - col_student)
            - 0.5 * (jnp.exp(t - row_t) + jnp.exp(t - col_teacher))
            - jnp.where(eye(b), 1.0, 0.0)
        ).astype(bf16)
        for j in range(K):
            gbuf[j, at, :] = grad[:, j * half : (j + 1) * half]
    if K > 1:
        send(gbuf.at[up(k, 1, K)], grecv, rg, partner)

    partial = 0.0
    for j in range(K):
        partial += jnp.dot(gbuf[j], txts[j * half : (j + 1) * half, :], preferred_element_type=f32)
    pi[...] = partial

    def first_hops(part, out_index, in_index, outer, inner, narrow, near, nears, slim, slims, direct, directs, joint, far, fars, target):
        for do in range(1, outer):
            there = up(out_index, do, outer)
            for di in range(inner):
                to = up(in_index, di, inner)
                value = piece(part, there * inner + to, 0)[...].astype(bf16)
                if di == 0:
                    src, dst, sem = piece(joint, do - 1, 0), piece(far, do - 1, 0), fars.at[do - 1, 0]
                else:
                    e = (do - 1) * (inner - 1) + di - 1
                    src, dst, sem = piece(slims, e, 0), piece(slim, e, 0), nears.at[e, 0]
                src[...] = value
                send(src, dst, sem, target(there, to))
        for j in range(1, S):
            for do in range(1, outer):
                for di in range(1, inner):
                    e = (do - 1) * (inner - 1) + di - 1
                    to = up(in_index, di, inner)
                    src = piece(part, up(out_index, do, outer) * inner + to, j)
                    if j % 2:
                        piece(slims, e, j)[...] = src[...].astype(bf16)
                        send(piece(slims, e, j), piece(slim, e, j), nears.at[e, j], target(out_index, to))
                    else:
                        send(src, piece(near, e, j), nears.at[e, j], target(out_index, to))
        for di in range(1, inner):
            to = up(in_index, di, inner)
            block(narrow, di - 1)[...] = block(part, out_index * inner + to)[...].astype(bf16)
            send(block(narrow, di - 1), block(direct, di - 1), directs.at[di - 1], target(out_index, to))

    def second_hops(part, out_index, in_index, outer, inner, near, nears, slim, joint, far, fars, target, j):
        for do in range(1, outer):
            to = up(out_index, do, outer)
            value = piece(part, to * inner + in_index, j)[...]
            for di in range(1, inner):
                e = (do - 1) * (inner - 1) + di - 1
                landed = piece(slim if j % 2 else near, e, j)
                arrived(landed, nears.at[e, j])
                value += landed[...].astype(f32)
            piece(joint, do - 1, j)[...] = value.astype(bf16)
            send(piece(joint, do - 1, j), piece(far, do - 1, j), fars.at[do - 1, j], target(to, in_index))

    def last_sum(out_ref, part, out_index, in_index, outer, inner, slim, nears, direct, directs, far, fars):
        value = block(part, out_index * inner + in_index)[...]
        for di in range(1, inner):
            arrived(block(direct, di - 1), directs.at[di - 1])
            value += block(direct, di - 1)[...].astype(f32)
        for do in range(1, outer):
            for j in range(S):
                arrived(piece(far, do - 1, j), fars.at[do - 1, j])
            value += block(far, do - 1)[...].astype(f32)
        out_ref[...] = logit_scale * value
        for e in range((outer - 1) * (inner - 1)):
            arrived(piece(slim, e, 0), nears.at[e, 0])
            out_ref[:m, :] += logit_scale * piece(slim, e, 0)[...].astype(f32)

    def image_target(p_, q_):
        return dev(r, hi, p_ * Q + q_, k)

    def text_target(h_, r_):
        return dev(r_, h_, lo, k)

    first_hops(pi, p, q, PP, Q, inarrow, inear, rinear, islim, islims, idirect, ridirect, ijoint, ifar, rifar, image_target)

    if K > 1:
        arrived(imgo, rimgo)
        arrived(grecv, rg)
    partial = contract_first(gbuf[k], imgs[...])
    if K > 1:
        partial += contract_first(grecv[...], imgo[...])
    pt[...] = partial
    first_hops(pt, hi, r, H, R, tnarrow, tnear, rtnear, tslim, tslims, tdirect, rtdirect, tjoint, tfar, rtfar, text_target)
    def loss_round():
        for d in range(1, A):
            arrived(la.at[d], rla.at[d])
        lb[0] = functools.reduce(jnp.add, [la[d] for d in range(A)])
        for e, target in enumerate(b_peers, 1):
            send(lb.at[0], lb.at[e], rlb.at[e], target)

    for j in range(1, S):
        second_hops(pi, p, q, PP, Q, inear, rinear, islim, ijoint, ifar, rifar, image_target, j)
        second_hops(pt, hi, r, H, R, tnear, rtnear, tslim, tjoint, tfar, rtfar, text_target, j)
        if j == 1:
            loss_round()
    if S == 1:
        loss_round()
    for e in range(1, T):
        arrived(lb.at[e], rlb.at[e])
    loss_ref[...] = functools.reduce(jnp.add, [lb[e] for e in range(T)]) / total
    last_sum(ig_ref, pi, p, q, PP, Q, islim, rinear, idirect, ridirect, ifar, rifar)
    last_sum(tg_ref, pt, hi, r, H, R, tslim, rtnear, tdirect, rtdirect, tfar, rtfar)
    for copy in pending:
        copy.wait_send()
    assert len(pending) == n_send, len(pending)


def leave(loss_in, image_in, text_in, loss_out, image_out, text_out, sems):
    image_copy = pltpu.make_async_copy(image_in, image_out, sems.at[0])
    text_copy = pltpu.make_async_copy(text_in, text_out, sems.at[1])
    image_copy.start()
    text_copy.start()
    loss_out[0, 0] = jnp.max(loss_in[...])
    image_copy.wait()
    text_copy.wait()


def solution(mesh):
    g = layout(mesh.shape)
    R, K, A, H, Q, PP = g["R"], g["K"], g["A"], g["H"], g["Q"], g["P"]
    HR, T = H * R, K * H * R
    near = ((PP - 1) * (Q - 1), (H - 1) * (R - 1))

    def body(image_student, text_student, image_teacher, text_teacher):
        n, width = image_student.shape
        rows, cols = A * n, T * n
        total = n * R * g["C"]
        S = g["S"] = 4 if n % 64 == 0 else 1
        gather = S * (2 * (A - 1) + 2 * (HR - 1) + 2 * HR * (K - 1)) + (K - 1)
        n_send = gather + 2 * (A - 1) + 2 * (T - 1) + (K - 1)
        n_send += S * (sum(near) + PP - 1 + H - 1) + Q - 1 + R - 1
        vmem, dma = pltpu.VMEM, pltpu.SemaphoreType.DMA

        def sums(size, near, direct, far):
            near, direct, far = max(near, 1) * n, max(direct, 1) * n, max(far, 1) * n
            return (
                vmem((size, width), f32), vmem((direct, width), bf16), vmem((near, width), f32),
                vmem((near, width), bf16), vmem((near, width), bf16),
                vmem((direct, width), bf16), vmem((far, width), bf16), vmem((far, width), bf16),
            )

        def arrivals(near, direct, far):
            return dma((max(near, 1), S)), dma((max(direct, 1),)), dma((max(far, 1), S))

        block_out = jax.ShapeDtypeStruct((n, width), f32)
        loss, image_grad, text_grad = pl.pallas_call(
            functools.partial(kernel, g, n_send, total),
            out_shape=(vmem((8, 128), f32), vmem((n, width), f32), vmem((n, width), f32)),
            in_specs=[pl.BlockSpec(memory_space=pl.ANY)] * 4,
            out_specs=[pl.BlockSpec(memory_space=pltpu.VMEM)] * 3,
            scratch_shapes=[
                vmem((rows, width), bf16), vmem((rows, width), bf16), vmem((rows, width), bf16),
                vmem((cols, width), bf16), vmem((cols, width), bf16),
                vmem((rows, cols), f32), vmem((rows, cols), f32),
                vmem((rows, 128), f32), vmem((A, 8, rows), f32), vmem((T, 8, cols), f32),
                vmem((A, 8, 128), f32), vmem((T, 8, 128), f32),
                vmem((K, rows, cols // K), bf16), vmem((rows, cols // K), bf16),
                *sums(rows, near[0], Q - 1, PP - 1), *sums(cols // K, near[1], R - 1, H - 1),
                dma((4,)), dma((n_send,)),
                dma((A, S)), dma(()), dma((A, S)), dma((T, S)), dma((T, S)),
                dma((A,)), dma((T,)), dma((A,)), dma((T,)), dma(()),
                *arrivals(near[0], Q - 1, PP - 1), *arrivals(near[1], R - 1, H - 1),
            ],
            compiler_params=pltpu.CompilerParams(
                collective_id=0, has_side_effects=True, vmem_limit_bytes=56 * 1024 * 1024
            ),
        )(image_student, text_student, image_teacher, text_teacher)
        loss, image_grad, text_grad = pl.pallas_call(
            leave,
            out_shape=(jax.ShapeDtypeStruct((1, 1), f32), block_out, block_out),
            in_specs=[pl.BlockSpec(memory_space=pltpu.VMEM)] * 3,
            out_specs=[pl.BlockSpec(memory_space=pltpu.SMEM)] + [pl.BlockSpec(memory_space=pl.ANY)] * 2,
            scratch_shapes=[dma((2,))],
            compiler_params=pltpu.CompilerParams(vmem_limit_bytes=1024 * 1024),
        )(loss, image_grad, text_grad)
        return loss[0, 0], image_grad, text_grad

    return jax.shard_map(
        body,
        mesh=mesh,
        in_specs=(
            P(("row", "col"), None),
            P(("col", "row"), None),
            P(("row", "col"), None),
            P(("col", "row"), None),
        ),
        out_specs=(P(), P(("row", "col"), None), P(("col", "row"), None)),
        check_vma=False,
    )
```

```python
import functools

import jax
import jax.numpy as jnp
from jax import lax
from jax.experimental import pallas as pl
from jax.experimental.pallas import tpu as pltpu
from jax.sharding import PartitionSpec as P

logit_scale = 100.0
MESH = pl.DeviceIdType.MESH
f32, bf16 = jnp.float32, jnp.bfloat16


def layout(mesh_shape):
    rows, cols = mesh_shape["row"], mesh_shape["col"]
    cores = 2 if cols % 2 == 0 else 1
    chips = cols // cores
    divisors = [d for d in range(1, chips + 1) if chips % d == 0]
    a = min(divisors, key=lambda d: d + rows * chips // d)
    q = max(d for d in range(1, a + 1) if a % d == 0 and d * d <= a)
    return dict(R=rows, C=cols, K=cores, A=a, H=chips // a, Q=q, P=a // q)


def contract_last(left, right):
    return lax.dot_general(left, right, (((1,), (1,)), ((), ())), preferred_element_type=f32)


def contract_first(left, right):
    return lax.dot_general(left, right, (((0,), (0,)), ((), ())), preferred_element_type=f32)


def merged(slots, count):
    def line(index, which):
        return slots[index, which : which + 1, :]

    student_high = functools.reduce(jnp.maximum, [line(i, 0) for i in range(count)])
    teacher_high = functools.reduce(jnp.maximum, [line(i, 2) for i in range(count)])
    student_total = teacher_total = divergence = 0.0
    for i in range(count):
        student_total += line(i, 1) * jnp.exp(line(i, 0) - student_high)
        factor = jnp.exp(line(i, 2) - teacher_high)
        teacher_total += line(i, 3) * factor
        divergence += line(i, 4) * factor
    student_lse = student_high + jnp.log(student_total)
    teacher_lse = teacher_high + jnp.log(teacher_total)
    kl = divergence / teacher_total - teacher_lse + student_lse
    return student_lse, teacher_lse, 0.5 * (student_lse + kl)


def position(index, step, count):
    total = jnp.zeros_like(index)
    for t in range(1, count):
        total += (index >= t * step).astype(jnp.int32)
    return total


def kernel(
    g, n_send, total,
    is_hbm, ts_hbm, it_hbm, tt_hbm,
    loss_ref, ig_ref, tg_ref,
    imgs, imgo, imgt, txts, txtt,
    s_ref, t_ref, rowtmp, rstat, cstat, la, lb, gbuf, grecv,
    pi, inarrow, inear, islim, islims, idirect, ijoint, ifar,
    pt, tnarrow, tnear, tslim, tslims, tdirect, tjoint, tfar,
    local_sem, send_sem, rimgs, rimgo, rimgt, rtxts, rtxtt, rrow, rcol, rla, rlb, rg,
    rinear, ridirect, rifar, rtnear, rtdirect, rtfar,
):
    R, K, A, H, Q, PP = g["R"], g["K"], g["A"], g["H"], g["Q"], g["P"]
    n, S = is_hbm.shape[0], g["S"]
    m = n // S
    r = lax.axis_index("row")
    c = lax.axis_index("col")
    k, chip = lax.rem(c, K), lax.div(c, K)
    lo, hi = lax.rem(chip, A), lax.div(chip, A)
    q, p = lax.rem(lo, Q), lax.div(lo, Q)
    HR, T = H * R, K * H * R

    def dev(r_, hi_, lo_, k_):
        return (r_, (hi_ * A + lo_) * K + k_)

    def up(value, step, count):
        return lax.rem(value + step, count)

    def down(value, step, count):
        return lax.rem(value + count - step, count)

    def block(ref, index):
        return ref.at[pl.ds(pl.multiple_of(index * n, n), n), :]

    def piece(ref, index, j):
        return ref.at[pl.ds(pl.multiple_of(index * n + j * m, m), m), :]

    a_peers = [dev(r, hi, up(lo, d, A), k) for d in range(1, A)]
    b_steps = [(dk, dh, dr) for dk in range(K) for dh in range(H) for dr in range(R)]
    b_peers = [dev(up(r, dr, R), up(hi, dh, H), lo, up(k, dk, K)) for dk, dh, dr in b_steps[1:]]
    partner = dev(r, hi, lo, up(k, 1, K))

    pending = []

    def send(src, dst, recv, target):
        copy = pltpu.make_async_remote_copy(
            src_ref=src, dst_ref=dst, send_sem=send_sem.at[len(pending)], recv_sem=recv,
            device_id=target, device_id_type=MESH,
        )
        copy.start()
        pending.append(copy)

    def arrived(ref, recv):
        pltpu.make_async_remote_copy(
            src_ref=ref, dst_ref=ref, send_sem=send_sem.at[0], recv_sem=recv,
            device_id=partner, device_id_type=MESH,
        ).wait_recv()

    own_text = (k * H + hi) * R + r
    loads = []
    for i, (src, dst) in enumerate((
        (is_hbm, block(imgs, lo)), (ts_hbm, block(txts, own_text)),
        (it_hbm, block(imgt, lo)), (tt_hbm, block(txtt, own_text)),
    )):
        copy = pltpu.make_async_copy(src, dst, local_sem.at[i])
        copy.start()
        loads.append(copy)
    barrier = pltpu.get_barrier_semaphore()
    for target in a_peers + b_peers:
        pl.semaphore_signal(barrier, inc=1, device_id=target, device_id_type=MESH)
    pl.semaphore_wait(barrier, len(a_peers) + len(b_peers))

    def image_slot(dp, dq):
        return down(p, dp, PP) * Q + down(q, dq, Q)

    def text_slot(dk, dh, dr):
        return (down(k, dk, K) * H + down(hi, dh, H)) * R + down(r, dr, R)

    def text_at(dk, dh, dr):
        return (dk * H + dh) * R + dr

    def image_own(ref, sems, j):
        for dp in range(1, PP):
            send(piece(ref, lo, j), piece(ref, lo, j), sems.at[dp * Q, j],
                 dev(r, hi, up(p, dp, PP) * Q + q, k))

    def image_spread(ref, sems, dp, j):
        slot = image_slot(dp, 0)
        for dq in range(1, Q):
            send(piece(ref, slot, j), piece(ref, slot, j), sems.at[dp * Q + dq, j],
                 dev(r, hi, p * Q + up(q, dq, Q), k))

    def text_own(ref, sems, j):
        for dh in range(1, H):
            send(piece(ref, own_text, j), piece(ref, own_text, j), sems.at[text_at(0, dh, 0), j],
                 dev(r, up(hi, dh, H), lo, k))

    def text_spread(ref, sems, dh, j):
        slot = text_slot(0, dh, 0)
        for dr in range(1, R):
            send(piece(ref, slot, j), piece(ref, slot, j), sems.at[text_at(0, dh, dr), j],
                 dev(up(r, dr, R), hi, lo, k))

    def text_across(ref, sems, dh, dr, j):
        slot = text_slot(0, dh, dr)
        for dk in range(1, K):
            send(piece(ref, slot, j), piece(ref, slot, j), sems.at[text_at(dk, dh, dr), j],
                 dev(r, hi, lo, up(k, dk, K)))

    pairs = ((imgs, rimgs, txts, rtxts), (imgt, rimgt, txtt, rtxtt))
    for i, (img, rimg, txt, rtxt) in enumerate(pairs):
        loads[2 * i].wait()
        loads[2 * i + 1].wait()
        for j in range(S):
            image_own(img, rimg, j)
            text_own(txt, rtxt, j)
        for j in range(S):
            image_spread(img, rimg, 0, j)
            text_spread(txt, rtxt, 0, j)
            text_across(txt, rtxt, 0, 0, j)

    def forward(img, rimg, txt, rtxt):
        for j in range(S):
            for dp in range(1, PP):
                arrived(piece(img, image_slot(dp, 0), j), rimg.at[dp * Q, j])
                image_spread(img, rimg, dp, j)
            for dh in range(1, H):
                arrived(piece(txt, text_slot(0, dh, 0), j), rtxt.at[text_at(0, dh, 0), j])
                text_spread(txt, rtxt, dh, j)
                text_across(txt, rtxt, dh, 0, j)

    def collect(img, rimg, txt, rtxt):
        for dh in range(H):
            for j in range(S):
                for dr in range(1, R):
                    arrived(piece(txt, text_slot(0, dh, dr), j), rtxt.at[text_at(0, dh, dr), j])
                    text_across(txt, rtxt, dh, dr, j)
        for j in range(S):
            for dp in range(PP):
                for dq in range(1, Q):
                    arrived(piece(img, image_slot(dp, dq), j), rimg.at[dp * Q + dq, j])
            for dk, dh, dr in b_steps:
                if dk:
                    arrived(piece(txt, text_slot(dk, dh, dr), j), rtxt.at[text_at(dk, dh, dr), j])

    for pair in pairs:
        forward(*pair)
    collect(*pairs[0])
    s_ref[...] = logit_scale * contract_last(imgs[...], txts[...])
    rows, width = s_ref.shape
    lane = lax.broadcasted_iota(jnp.int32, (n, 128), 1)
    col_id = lax.broadcasted_iota(jnp.int32, (1, width), 1)
    col_slot = position(col_id, n, T)
    slot_k, slot_h = position(col_slot, HR, K), position(col_slot, R, K * H)
    slot_r = col_slot - slot_h * R
    slot_h = slot_h - slot_k * H
    col_id = (((slot_h * A + lo) * K + slot_k) * R + slot_r) * n + col_id - col_slot * n
    row_id = lax.broadcasted_iota(jnp.int32, (n, 1), 0)

    def eye(b):
        base = (r * g["C"] + (hi * A + b) * K + k) * n
        return row_id + base == col_id

    def pack(values, into, index):
        for i, value in values:
            into = jnp.where(index == i, value, into)
        return into

    col_s = jnp.max(s_ref[...], axis=0, keepdims=True)
    col_total = diagonal = 0.0
    for b in range(A):
        at = slice(b * n, (b + 1) * n)
        s = s_ref[at, :]
        row_s = jnp.max(s, axis=1, keepdims=True)
        row_total = jnp.sum(jnp.exp(s - row_s), axis=1, keepdims=True)
        rowtmp[at, :] = pack(((0, row_s), (1, row_total)), jnp.zeros((n, 128), f32), lane)
        col_total += jnp.sum(jnp.exp(s - col_s), axis=0, keepdims=True)
        diagonal += jnp.sum(jnp.where(eye(b), s, 0.0), axis=0, keepdims=True)
    collect(*pairs[1])
    if K > 1:
        send(imgs, imgo, rimgo, partner)
    t_ref[...] = logit_scale * contract_last(imgt[...], txtt[...])

    col_t = jnp.max(t_ref[...], axis=0, keepdims=True)
    sums = [0.0] * 2
    for b in range(A):
        at = slice(b * n, (b + 1) * n)
        s, t = s_ref[at, :], t_ref[at, :]
        gap = t - s
        row_t = jnp.max(t, axis=1, keepdims=True)
        row_weight = jnp.exp(t - row_t)
        row_sums = [jnp.sum(v, axis=1, keepdims=True) for v in (row_weight, row_weight * gap)]
        rowtmp[at, :] = pack(((2, row_t), (3, row_sums[0]), (4, row_sums[1])), rowtmp[at, :], lane)
        col_weight = jnp.exp(t - col_t)
        sums = [
            old + jnp.sum(new, axis=0, keepdims=True)
            for old, new in zip(sums, (col_weight, col_weight * gap))
        ]
    line = lax.broadcasted_iota(jnp.int32, (8, width), 0)
    packed = pack(enumerate((col_s, col_total, col_t, *sums)), jnp.zeros((8, width), f32), line)
    cstat[0] = packed
    for e, target in enumerate(b_peers, 1):
        send(cstat.at[0], cstat.at[e], rcol.at[e], target)
    rstat[0] = jnp.transpose(rowtmp[...])[:8, :]
    for d, target in enumerate(a_peers, 1):
        send(rstat.at[0], rstat.at[d], rrow.at[d], target)
    for d in range(1, A):
        arrived(rstat.at[d], rrow.at[d])
    row_student, row_teacher, row_terms = merged(rstat, A)
    line = lax.broadcasted_iota(jnp.int32, (128, rows), 0)
    rowtmp[...] = jnp.transpose(jnp.where(line == 0, row_student, row_teacher))
    for e in range(1, T):
        arrived(cstat.at[e], rcol.at[e])
    col_student, col_teacher, col_terms = merged(cstat, T)

    at_row = lax.broadcasted_iota(jnp.int32, (1, rows), 1) - lo * n
    at_col = lax.broadcasted_iota(jnp.int32, (1, width), 1) - own_text * n
    share = (
        jnp.sum(jnp.where((at_row >= 0) & (at_row < n), row_terms, 0.0), axis=1, keepdims=True)
        + jnp.sum(
            jnp.where((at_col >= 0) & (at_col < n), col_terms, 0.0) - diagonal,
            axis=1, keepdims=True,
        )
    )
    la[0] = jnp.broadcast_to(share, (8, 128))
    for d, target in enumerate(a_peers, 1):
        send(la.at[0], la.at[d], rla.at[d], target)

    half = width // K
    for b in range(A):
        at = slice(b * n, (b + 1) * n)
        s, t = s_ref[at, :], t_ref[at, :]
        row_s, row_t = rowtmp[at, 0:1], rowtmp[at, 1:2]
        grad = (
            jnp.exp(s - row_s) + jnp.exp(s - col_student)
            - 0.5 * (jnp.exp(t - row_t) + jnp.exp(t - col_teacher))
            - jnp.where(eye(b), 1.0, 0.0)
        ).astype(bf16)
        for j in range(K):
            gbuf[j, at, :] = grad[:, j * half : (j + 1) * half]
    if K > 1:
        send(gbuf.at[up(k, 1, K)], grecv, rg, partner)

    partial = 0.0
    for j in range(K):
        partial += jnp.dot(gbuf[j], txts[j * half : (j + 1) * half, :], preferred_element_type=f32)
    pi[...] = partial

    def first_hops(part, out_index, in_index, outer, inner, narrow, near, nears, slim, slims, direct, directs, joint, far, fars, target):
        for do in range(1, outer):
            there = up(out_index, do, outer)
            for di in range(inner):
                to = up(in_index, di, inner)
                value = piece(part, there * inner + to, 0)[...].astype(bf16)
                if di == 0:
                    src, dst, sem = piece(joint, do - 1, 0), piece(far, do - 1, 0), fars.at[do - 1, 0]
                else:
                    e = (do - 1) * (inner - 1) + di - 1
                    src, dst, sem = piece(slims, e, 0), piece(slim, e, 0), nears.at[e, 0]
                src[...] = value
                send(src, dst, sem, target(there, to))
        for j in range(1, S):
            for do in range(1, outer):
                for di in range(1, inner):
                    e = (do - 1) * (inner - 1) + di - 1
                    to = up(in_index, di, inner)
                    src = piece(part, up(out_index, do, outer) * inner + to, j)
                    if j % 2:
                        piece(slims, e, j)[...] = src[...].astype(bf16)
                        send(piece(slims, e, j), piece(slim, e, j), nears.at[e, j], target(out_index, to))
                    else:
                        send(src, piece(near, e, j), nears.at[e, j], target(out_index, to))
        for di in range(1, inner):
            to = up(in_index, di, inner)
            block(narrow, di - 1)[...] = block(part, out_index * inner + to)[...].astype(bf16)
            send(block(narrow, di - 1), block(direct, di - 1), directs.at[di - 1], target(out_index, to))

    def second_hops(part, out_index, in_index, outer, inner, near, nears, slim, joint, far, fars, target, j):
        for do in range(1, outer):
            to = up(out_index, do, outer)
            value = piece(part, to * inner + in_index, j)[...]
            for di in range(1, inner):
                e = (do - 1) * (inner - 1) + di - 1
                landed = piece(slim if j % 2 else near, e, j)
                arrived(landed, nears.at[e, j])
                value += landed[...].astype(f32)
            piece(joint, do - 1, j)[...] = value.astype(bf16)
            send(piece(joint, do - 1, j), piece(far, do - 1, j), fars.at[do - 1, j], target(to, in_index))

    def last_sum(out_ref, part, out_index, in_index, outer, inner, slim, nears, direct, directs, far, fars):
        value = block(part, out_index * inner + in_index)[...]
        for di in range(1, inner):
            arrived(block(direct, di - 1), directs.at[di - 1])
            value += block(direct, di - 1)[...].astype(f32)
        for do in range(1, outer):
            for j in range(S):
                arrived(piece(far, do - 1, j), fars.at[do - 1, j])
            value += block(far, do - 1)[...].astype(f32)
        out_ref[...] = logit_scale * value
        for e in range((outer - 1) * (inner - 1)):
            arrived(piece(slim, e, 0), nears.at[e, 0])
            out_ref[:m, :] += logit_scale * piece(slim, e, 0)[...].astype(f32)

    def image_target(p_, q_):
        return dev(r, hi, p_ * Q + q_, k)

    def text_target(h_, r_):
        return dev(r_, h_, lo, k)

    first_hops(pi, p, q, PP, Q, inarrow, inear, rinear, islim, islims, idirect, ridirect, ijoint, ifar, rifar, image_target)

    pt[...] = contract_first(gbuf[k], imgs[...])
    if K > 1:
        arrived(imgo, rimgo)
        arrived(grecv, rg)
        pt[...] += contract_first(grecv[...], imgo[...])
    first_hops(pt, hi, r, H, R, tnarrow, tnear, rtnear, tslim, tslims, tdirect, rtdirect, tjoint, tfar, rtfar, text_target)
    def loss_round():
        for d in range(1, A):
            arrived(la.at[d], rla.at[d])
        lb[0] = functools.reduce(jnp.add, [la[d] for d in range(A)])
        for e, target in enumerate(b_peers, 1):
            send(lb.at[0], lb.at[e], rlb.at[e], target)

    for j in range(1, S):
        second_hops(pi, p, q, PP, Q, inear, rinear, islim, ijoint, ifar, rifar, image_target, j)
        second_hops(pt, hi, r, H, R, tnear, rtnear, tslim, tjoint, tfar, rtfar, text_target, j)
        if j == 1:
            loss_round()
    if S == 1:
        loss_round()
    for e in range(1, T):
        arrived(lb.at[e], rlb.at[e])
    loss_ref[...] = functools.reduce(jnp.add, [lb[e] for e in range(T)]) / total
    last_sum(ig_ref, pi, p, q, PP, Q, islim, rinear, idirect, ridirect, ifar, rifar)
    last_sum(tg_ref, pt, hi, r, H, R, tslim, rtnear, tdirect, rtdirect, tfar, rtfar)
    for copy in pending:
        copy.wait_send()
    assert len(pending) == n_send, len(pending)


def leave(loss_in, image_in, text_in, loss_out, image_out, text_out, sems):
    image_copy = pltpu.make_async_copy(image_in, image_out, sems.at[0])
    text_copy = pltpu.make_async_copy(text_in, text_out, sems.at[1])
    image_copy.start()
    text_copy.start()
    loss_out[0, 0] = jnp.max(loss_in[...])
    image_copy.wait()
    text_copy.wait()


def solution(mesh):
    g = layout(mesh.shape)
    R, K, A, H, Q, PP = g["R"], g["K"], g["A"], g["H"], g["Q"], g["P"]
    HR, T = H * R, K * H * R
    near = ((PP - 1) * (Q - 1), (H - 1) * (R - 1))

    def body(image_student, text_student, image_teacher, text_teacher):
        n, width = image_student.shape
        rows, cols = A * n, T * n
        total = n * R * g["C"]
        S = g["S"] = 4 if n % 64 == 0 else 1
        gather = S * (2 * (A - 1) + 2 * (HR - 1) + 2 * HR * (K - 1)) + (K - 1)
        n_send = gather + 2 * (A - 1) + 2 * (T - 1) + (K - 1)
        n_send += S * (sum(near) + PP - 1 + H - 1) + Q - 1 + R - 1
        vmem, dma = pltpu.VMEM, pltpu.SemaphoreType.DMA

        def sums(size, near, direct, far):
            near, direct, far = max(near, 1) * n, max(direct, 1) * n, max(far, 1) * n
            return (
                vmem((size, width), f32), vmem((direct, width), bf16), vmem((near, width), f32),
                vmem((near, width), bf16), vmem((near, width), bf16),
                vmem((direct, width), bf16), vmem((far, width), bf16), vmem((far, width), bf16),
            )

        def arrivals(near, direct, far):
            return dma((max(near, 1), S)), dma((max(direct, 1),)), dma((max(far, 1), S))

        block_out = jax.ShapeDtypeStruct((n, width), f32)
        loss, image_grad, text_grad = pl.pallas_call(
            functools.partial(kernel, g, n_send, total),
            out_shape=(vmem((8, 128), f32), vmem((n, width), f32), vmem((n, width), f32)),
            in_specs=[pl.BlockSpec(memory_space=pl.ANY)] * 4,
            out_specs=[pl.BlockSpec(memory_space=pltpu.VMEM)] * 3,
            scratch_shapes=[
                vmem((rows, width), bf16), vmem((rows, width), bf16), vmem((rows, width), bf16),
                vmem((cols, width), bf16), vmem((cols, width), bf16),
                vmem((rows, cols), f32), vmem((rows, cols), f32),
                vmem((rows, 128), f32), vmem((A, 8, rows), f32), vmem((T, 8, cols), f32),
                vmem((A, 8, 128), f32), vmem((T, 8, 128), f32),
                vmem((K, rows, cols // K), bf16), vmem((rows, cols // K), bf16),
                *sums(rows, near[0], Q - 1, PP - 1), *sums(cols // K, near[1], R - 1, H - 1),
                dma((4,)), dma((n_send,)),
                dma((A, S)), dma(()), dma((A, S)), dma((T, S)), dma((T, S)),
                dma((A,)), dma((T,)), dma((A,)), dma((T,)), dma(()),
                *arrivals(near[0], Q - 1, PP - 1), *arrivals(near[1], R - 1, H - 1),
            ],
            compiler_params=pltpu.CompilerParams(
                collective_id=0, has_side_effects=True, vmem_limit_bytes=56 * 1024 * 1024
            ),
        )(image_student, text_student, image_teacher, text_teacher)
        loss, image_grad, text_grad = pl.pallas_call(
            leave,
            out_shape=(jax.ShapeDtypeStruct((1, 1), f32), block_out, block_out),
            in_specs=[pl.BlockSpec(memory_space=pltpu.VMEM)] * 3,
            out_specs=[pl.BlockSpec(memory_space=pltpu.SMEM)] + [pl.BlockSpec(memory_space=pl.ANY)] * 2,
            scratch_shapes=[dma((2,))],
            compiler_params=pltpu.CompilerParams(vmem_limit_bytes=1024 * 1024),
        )(loss, image_grad, text_grad)
        return loss[0, 0], image_grad, text_grad

    return jax.shard_map(
        body,
        mesh=mesh,
        in_specs=(
            P(("row", "col"), None),
            P(("col", "row"), None),
            P(("row", "col"), None),
            P(("col", "row"), None),
        ),
        out_specs=(P(), P(("row", "col"), None), P(("col", "row"), None)),
        check_vma=False,
    )
```
